128 devices in a mesh: rep: 1, dp: 128 (over x, y, z, core).
Axes of the slice: x: 4, y: 4, z: 4, core: 2. Of those that a mesh axis runs over, the one named last changes fastest.
Arguments:
- x: bfloat16 [128, 1024, 512], P(('rep', 'dp'))
- dy: bfloat16 [128, 1024, 512], P(('rep', 'dp'))
- wq: bfloat16 [1, 512, 2048], replicated
- wk: bfloat16 [1, 512, 2048], replicated
- wv: bfloat16 [1, 512, 2048], replicated
- wo: bfloat16 [1, 2048, 512], replicated
- w_gate: bfloat16 [1, 512, 8192], replicated
- w_up: bfloat16 [1, 512, 8192], replicated
- w_down: bfloat16 [1, 8192, 512], replicated
- m_wq: float32 [1, 512, 2048], replicated
- m_wk: float32 [1, 512, 2048], replicated
- m_wv: float32 [1, 512, 2048], replicated
- m_wo: float32 [1, 2048, 512], replicated
- m_w_gate: float32 [1, 512, 8192], replicated
- m_w_up: float32 [1, 512, 8192], replicated
- m_w_down: float32 [1, 8192, 512], replicated
- v_wq: float32 [1, 512, 2048], replicated
- v_wk: float32 [1, 512, 2048], replicated
- v_wv: float32 [1, 512, 2048], replicated
- v_wo: float32 [1, 2048, 512], replicated
- v_w_gate: float32 [1, 512, 8192], replicated
- v_w_up: float32 [1, 512, 8192], replicated
- v_w_down: float32 [1, 8192, 512], replicated
Outputs:
- output 1: bfloat16 [1, 512, 2048], P('rep')
- output 2: bfloat16 [1, 512, 2048], P('rep')
- output 3: bfloat16 [1, 512, 2048], P('rep')
- output 4: bfloat16 [1, 2048, 512], P('rep')
- output 5: bfloat16 [1, 512, 8192], P('rep')
- output 6: bfloat16 [1, 512, 8192], P('rep')
- output 7: bfloat16 [1, 8192, 512], P('rep')
- output 8: float32 [1, 512, 2048], P('rep')
- output 9: float32 [1, 512, 2048], P('rep')
- output 10: float32 [1, 512, 2048], P('rep')
- output 11: float32 [1, 2048, 512], P('rep')
- output 12: float32 [1, 512, 8192], P('rep')
- output 13: float32 [1, 512, 8192], P('rep')
- output 14: float32 [1, 8192, 512], P('rep')
- output 15: float32 [1, 512, 2048], P('rep')
- output 16: float32 [1, 512, 2048], P('rep')
- output 17: float32 [1, 512, 2048], P('rep')
- output 18: float32 [1, 2048, 512], P('rep')
- output 19: float32 [1, 512, 8192], P('rep')
- output 20: float32 [1, 512, 8192], P('rep')
- output 21: float32 [1, 8192, 512], P('rep')
All inputs are finite; a program needn't handle non-finite values.
Results may differ from the reference program's by a relative error of at most 0.024.
Values are sent between devices in bfloat16 or wider.
A program may use at most 1.5 GiB of HBM per device.

```python
import jax
import jax.numpy as jnp
from jax import lax

SEQUENCES = 128
TOKENS = 1024
D = 512
HEADS = 16
KV_HEADS = 16
HEAD = 128
FF = 8192
LAYERS = 1
THETA = 10000
NAMES = ("wq", "wk", "wv", "wo", "w_gate", "w_up", "w_down")
SHAPES = {
    "wq": (LAYERS, D, HEADS * HEAD),
    "wk": (LAYERS, D, KV_HEADS * HEAD),
    "wv": (LAYERS, D, KV_HEADS * HEAD),
    "wo": (LAYERS, HEADS * HEAD, D),
    "w_gate": (LAYERS, D, FF),
    "w_up": (LAYERS, D, FF),
    "w_down": (LAYERS, FF, D),
}


def bump(key, n, height):
    away = (jnp.arange(n, dtype=jnp.int32) - jax.random.randint(key, (), 0, n, jnp.int32)) % n
    return jnp.where(away < n // 8, height, 1.0)


def together(key, own, strength):
    shared = jax.random.normal(key, own.shape[1:], jnp.float32)
    return (own + strength * shared) * lax.rsqrt(1 + strength * strength)


def setup_inputs(seed: int = 0, part: int = 0) -> dict:
    kx, kdy, ka, kb, kz, kf, kh, kl, *keys = jax.random.split(jax.random.key(seed), 8 + 3 * len(NAMES))
    kx, kdy, ka, kb = (jax.random.fold_in(k, part) for k in (kx, kdy, ka, kb))
    kw, km, kv = (keys[i::3] for i in range(3))
    shape = (SEQUENCES, TOKENS, D)
    much_x, much_dy = jax.random.uniform(kz, (2,), jnp.float32, 0.0, 1.0)
    loud = 2.0 ** jax.random.uniform(jax.random.fold_in(kz, 1), (), jnp.float32, -1.0, 2.0)
    layers = 2.0 ** jax.random.uniform(kl, (LAYERS, 1, 1), jnp.float32, -1.0, 1.0)
    times = {"wq": 1.0, "wk": 1.0, "wv": 2.0, "wo": layers, "w_gate": 1.0, "w_up": bump(kh, FF, 4.0), "w_down": layers}
    x = together(ka, jax.random.normal(kx, shape, jnp.float32), much_x) * bump(kf, D, 4.0)
    dy = together(kb, jax.random.normal(kdy, shape, jnp.float32), much_dy)
    drawn = {"x": x.astype(jnp.bfloat16), "dy": (loud * dy * (SEQUENCES * TOKENS) ** -0.5).astype(jnp.bfloat16)}
    for key, name in zip(kw, NAMES, strict=True):
        drawn[name] = (jax.random.normal(key, SHAPES[name], jnp.float32) * SHAPES[name][1] ** -0.5 * times[name]).astype(jnp.bfloat16)
    for key, name in zip(km, NAMES, strict=True):
        drawn[f"m_{name}"] = 0.1 * jax.random.normal(key, SHAPES[name], jnp.float32)
    for key, name in zip(kv, NAMES, strict=True):
        drawn[f"v_{name}"] = jax.random.uniform(key, SHAPES[name], jnp.float32, 0.02, 0.06)
    return drawn


def matmul(a, w):
    return jnp.dot(a, w, preferred_element_type=jnp.float32).astype(jnp.bfloat16)


def normed(h):
    wide = h.astype(jnp.float32)
    scale = lax.rsqrt(jnp.mean(wide**2, -1, keepdims=True) + 1e-6)
    return (wide * scale).astype(jnp.bfloat16)


def turned(t, theta):
    half = t.shape[-1] // 2
    angle = jnp.arange(t.shape[0], dtype=jnp.float32)[:, None] * theta ** (-jnp.arange(half, dtype=jnp.float32) / half)
    cos, sin = jnp.cos(angle)[:, None], jnp.sin(angle)[:, None]
    a, b = t[..., :half].astype(jnp.float32), t[..., half:].astype(jnp.float32)
    return jnp.concatenate([a * cos - b * sin, b * cos + a * sin], -1).astype(jnp.bfloat16)


def seen_by(q, k, v):
    tokens, kv = q.shape[0], k.shape[1]
    q = q.reshape(tokens, kv, -1, q.shape[-1])
    scores = jnp.einsum("tgsd,ugd->gstu", q.astype(jnp.float32), k.astype(jnp.float32)) * q.shape[-1] ** -0.5
    place = jnp.arange(tokens)
    weights = jax.nn.softmax(jnp.where(place[:, None] >= place, scores, -jnp.inf), -1).astype(jnp.bfloat16)
    return jnp.einsum("gstu,ugd->tgsd", weights.astype(jnp.float32), v.astype(jnp.float32)).astype(jnp.bfloat16).reshape(tokens, -1)


def layer(h, w):
    a = normed(h)
    q, k = (turned(matmul(a, w[name]).reshape(h.shape[0], -1, HEAD), THETA) for name in ("wq", "wk"))
    h = h + matmul(seen_by(q, k, matmul(a, w["wv"]).reshape(h.shape[0], -1, HEAD)), w["wo"])
    b = normed(h)
    gate = jnp.dot(b, w["w_gate"], preferred_element_type=jnp.float32)
    up = jnp.dot(b, w["w_up"], preferred_element_type=jnp.float32)
    return h + matmul((jax.nn.silu(gate) * up).astype(jnp.bfloat16), w["w_down"])


def adamw(w, m, v, g):
    m = 0.9 * m + 0.1 * g
    v = 0.95 * v + 0.05 * g * g
    step = m * lax.rsqrt(v + 1e-8) + 0.1 * w
    return (w - 0.02 * step).astype(jnp.bfloat16), m, v


def clipped(gradients, sum_of_squares, count):
    factor = jnp.minimum(1.0, 0.5 * lax.rsqrt(sum_of_squares / count + 1e-30))
    return [g * factor for g in gradients]


def stack(weights, h):
    return lax.scan(lambda h, w: (layer(h, w), None), h, weights)[0]


def reference(x, dy, wq, wk, wv, wo, w_gate, w_up, w_down, m_wq, m_wk, m_wv, m_wo, m_w_gate, m_w_up, m_w_down, v_wq, v_wk, v_wv, v_wo, v_w_gate, v_w_up, v_w_down):
    weights = dict(zip(NAMES, (wq, wk, wv, wo, w_gate, w_up, w_down), strict=True))

    def take(so_far, sequence):
        h, by_y = sequence
        _, back = jax.vjp(stack, weights, h)
        by_weights, by_h = back(by_y)
        return jax.tree.map(lambda total, term: total + term.astype(jnp.float32), so_far, by_weights), by_h

    none_yet = {name: jnp.zeros(w.shape, jnp.float32) for name, w in weights.items()}
    by_weights, by_x = lax.scan(take, none_yet, (x, dy))
    gradients = [by_weights[name].astype(jnp.bfloat16).astype(jnp.float32) for name in NAMES]
    gradients = clipped(gradients, sum(jnp.sum(g * g) for g in gradients), sum(g.size for g in gradients))
    first = (m_wq, m_wk, m_wv, m_wo, m_w_gate, m_w_up, m_w_down)
    second = (v_wq, v_wk, v_wv, v_wo, v_w_gate, v_w_up, v_w_down)
    new = [adamw(weights[name].astype(jnp.float32), m, v, g) for name, m, v, g in zip(NAMES, first, second, gradients, strict=True)]
    return tuple(one[which] for which in range(3) for one in new)
```

```python
import functools
import jax, jax.numpy as jnp
from jax import lax
from jax.experimental import pallas as pl
from jax.experimental.pallas import tpu as pltpu
from jax.sharding import PartitionSpec as P

F32, BF16 = jnp.float32, jnp.bfloat16
NEG = -1e30
HIDDEN = 2 * NEG
LOG2E = 1.4426950408889634
D, HALF, HEAD, QUARTER, EIGHTH, PIECE = 512, 256, 128, 64, 32, 16
THETA = 10000
VMEM = 58 * 2**20
NAMES = ("wq", "wk", "wv", "wo", "w_gate", "w_up", "w_down")
CHUNKS = 64
LARGE = 48
ANY = "arbitrary"


def _dot(a, b, ca=1, cb=0):
    return lax.dot_general(a, b, (((ca,), (cb,)), ((), ())), preferred_element_type=F32)


def _params(*semantics):
    return pltpu.CompilerParams(dimension_semantics=semantics, vmem_limit_bytes=VMEM)


def _cost(flops, nbytes, exps=0):
    return pl.CostEstimate(flops=int(flops), bytes_accessed=int(nbytes), transcendentals=int(exps))


def tables(tokens):
    half = HEAD // 2
    angle = jnp.arange(tokens, dtype=F32)[:, None] * THETA ** (-jnp.arange(half, dtype=F32) / half)
    cos, sin = jnp.cos(angle), jnp.sin(angle)
    return jnp.concatenate([cos, cos], 1), jnp.concatenate([-sin, sin], 1)


def _qkv_kernel(x_ref, wq_ref, wk_ref, wv_ref, cos_ref, sin_ref, q_ref, k_ref, v_ref, at_ref, a_s):
    @pl.when(pl.program_id(0) == 0)
    def _():
        wide = x_ref[...].astype(F32)
        a_s[...] = (wide * lax.rsqrt(jnp.mean(wide * wide, -1, keepdims=True) + 1e-6)).astype(BF16)
        at_ref[...] = a_s[...].T

    for r in range(0, 1024, HALF):
        a = a_s[r : r + HALF]
        cos, sin = cos_ref[r : r + HALF], sin_ref[r : r + HALF]
        for w, out in ((wq_ref, q_ref), (wk_ref, k_ref)):
            t = _dot(a, w[0]).astype(BF16).astype(F32)
            for n in range(0, D, HEAD):
                one = t[:, n : n + HEAD]
                out[r : r + HALF, n : n + HEAD] = (one * cos + pltpu.roll(one, QUARTER, 1) * sin).astype(BF16)
        v_ref[r : r + HALF] = _dot(a, wv_ref[0]).astype(BF16)


def qkv(x, wq, wk, wv, cos, sin):
    t = x.shape[0]
    whole = lambda *s: pl.BlockSpec(s, lambda i: (0, 0))
    cols = pl.BlockSpec((t, D), lambda i: (0, i))
    w = pl.BlockSpec((1, D, D), lambda i: (0, 0, i))
    out = jax.ShapeDtypeStruct((t, 2048), BF16)
    return pl.pallas_call(
        _qkv_kernel, grid=(4,), in_specs=[whole(t, D), w, w, w, whole(t, HEAD), whole(t, HEAD)],
        out_specs=[cols, cols, cols, whole(D, t)], out_shape=[out, out, out, jax.ShapeDtypeStruct((D, t), BF16)],
        scratch_shapes=[pltpu.VMEM((t, D), BF16)], compiler_params=_params(ANY), cost_estimate=_cost(6.4e9, 2e7),
    )(x, wq, wk, wv, cos, sin)


BQ = HALF
BK = HALF


def _attend_kernel(q_ref, k_ref, v_ref, o_ref, ot_ref, lse_ref, top_s, mix_s, *, scale):
    iq = pl.program_id(0)
    e = scale * LOG2E
    heads = q_ref.shape[1] // HEAD
    col = lambda i: slice(i * HEAD, i * HEAD + HEAD)
    top_s[...] = jnp.full_like(top_s, NEG)
    mix_s[...] = jnp.zeros_like(mix_s)
    ones = jnp.ones((8, BK), BF16)
    hidden = lax.broadcasted_iota(jnp.int32, (BK, BQ), 0) > lax.broadcasted_iota(jnp.int32, (BK, BQ), 1)

    def block(j, masked):
        here = pl.ds(pl.multiple_of(j * BK, BK), BK)
        scores = [_dot(k_ref[here, col(i)], q_ref[:, col(i)], 1, 1) for i in range(heads)]
        weights, keeps = [], []
        for i, s in enumerate(scores):
            if masked:
                s = jnp.where(hidden, HIDDEN, s)
            old = top_s[i : i + 1, :]
            top = jnp.maximum(old, s.max(axis=0, keepdims=True))
            top_s[i : i + 1, :] = top
            weights.append(jnp.exp2((s - top) * e).astype(BF16))
            keeps.append(jnp.exp2((old - top) * e))
        for i, (p, keep) in enumerate(zip(weights, keeps)):
            values = jnp.concatenate([v_ref[here, col(i)].T, ones], axis=0)
            mix_s[i] = mix_s[i] * keep + _dot(values, p)

    lax.fori_loop(0, iq, lambda j, _: block(j, False), None)
    block(iq, True)
    for i in range(heads):
        total = mix_s[i, HEAD : HEAD + 1, :]
        out = (mix_s[i, :HEAD, :] * (1 / total)).astype(BF16)
        ot_ref[col(i), :] = out
        o_ref[:, col(i)] = out.T
        lse_ref[i : i + 1, :] = top_s[i : i + 1, :] * e + jnp.log2(total)


def attend(q, k, v):
    t, width = q.shape
    heads = width // HEAD
    rows = pl.BlockSpec((BQ, width), lambda i: (i, 0))
    whole = pl.BlockSpec((t, width), lambda i: (0, 0))
    return pl.pallas_call(
        functools.partial(_attend_kernel, scale=HEAD**-0.5), grid=(t // BQ,), in_specs=[rows, whole, whole],
        out_specs=[rows, pl.BlockSpec((width, BQ), lambda i: (0, i)), pl.BlockSpec((heads, BQ), lambda i: (0, i))],
        out_shape=[jax.ShapeDtypeStruct((t, width), BF16), jax.ShapeDtypeStruct((width, t), BF16), jax.ShapeDtypeStruct((heads, t), F32)],
        scratch_shapes=[pltpu.VMEM((heads, BQ), F32), pltpu.VMEM((heads, HEAD + 8, BQ), F32)],
        compiler_params=_params(ANY), cost_estimate=_cost(1e10, 2e7, 1e7),
    )(q, k, v)


def _mlp_kernel(x_ref, o_ref, wo_ref, dy_ref, wg_ref, wu_ref, wd_ref, dw_ref, dh_ref,
                b_s, bt_s, dyt_s, db_s, h_s, scale_s, hid_s, dg_s, du_s):
    i = pl.program_id(0)
    t = x_ref.shape[0]

    @pl.when(i == 0)
    def _():
        for r in range(0, t, HALF):
            here = slice(r, r + HALF)
            h = (x_ref[here].astype(F32) + _dot(o_ref[here], wo_ref[0]).astype(BF16).astype(F32)).astype(BF16)
            h_s[here] = h
            wide = h.astype(F32)
            scale = lax.rsqrt(jnp.mean(wide * wide, -1, keepdims=True) + 1e-6)
            scale_s[here] = jnp.broadcast_to(scale, (HALF, HEAD))
            b_s[here] = (wide * scale).astype(BF16)
        bt_s[...] = b_s[...].T
        dyt_s[...] = dy_ref[...].T
        db_s[...] = jnp.zeros_like(db_s)

    wg, wu, wd = wg_ref[0], wu_ref[0], wd_ref[0]
    for r in range(0, t, HALF):
        here = slice(r, r + HALF)
        gate, up = _dot(b_s[here], wg), _dot(b_s[here], wu)
        dh = _dot(dy_ref[here], wd, 1, 1).astype(BF16).astype(F32)
        sig = 0.5 * jnp.tanh(0.5 * gate) + 0.5
        act = gate * sig
        hid_s[here] = (act * up).astype(BF16)
        dup = (dh * act).astype(BF16)
        dgate = (dh * up * (sig + act * (1 - sig))).astype(BF16)
        du_s[here] = dup
        dg_s[here] = dgate
        db_s[here] += _dot(dgate, wg, 1, 1) + _dot(dup, wu, 1, 1)
    dw_ref[2] = _dot(dyt_s[...], hid_s[...]).astype(BF16)
    dw_ref[0] = _dot(bt_s[...], dg_s[...]).astype(BF16)
    dw_ref[1] = _dot(bt_s[...], du_s[...]).astype(BF16)

    @pl.when(i == pl.num_programs(0) - 1)
    def _():
        for r in range(0, t, HALF):
            here = slice(r, r + HALF)
            db = db_s[here].astype(BF16).astype(F32)
            wide, scale = h_s[here].astype(F32), scale_s[here][:, :1]
            inner = jnp.mean(db * wide, -1, keepdims=True)
            dh_ref[here] = (dy_ref[here].astype(F32) + (db * scale - wide * (scale * scale * scale * inner))).astype(BF16)


def mlp(x, o, wo, dy, wg, wu, wd):
    t = x.shape[0]
    n = wg.shape[2] // D
    whole = lambda a: pl.BlockSpec(a.shape, lambda i: (0,) * a.ndim)
    cols = pl.BlockSpec((1, D, D), lambda i: (0, 0, i))
    rows = pl.BlockSpec((1, D, D), lambda i: (0, i, 0))
    vm = pltpu.VMEM
    return pl.pallas_call(
        _mlp_kernel, grid=(n,), in_specs=[whole(x), whole(o), whole(wo), whole(dy), cols, cols, rows],
        out_specs=[pl.BlockSpec((3, D, D), lambda i: (i, 0, 0)), whole(x)],
        out_shape=[jax.ShapeDtypeStruct((CHUNKS, D, D), BF16), jax.ShapeDtypeStruct(x.shape, BF16)],
        scratch_shapes=[vm((t, D), BF16), vm((D, t), BF16), vm((D, t), BF16), vm((t, D), F32), vm((t, D), BF16), vm((t, HEAD), F32),
                        vm((t, D), BF16), vm((t, D), BF16), vm((t, D), BF16)],
        compiler_params=_params(ANY), cost_estimate=_cost(7.1e10, 6e7, 8e6),
    )(x, o, wo, dy, wg, wu, wd)


BQB = D
BKB = HALF


def _attend_bwd_kernel(q_ref, k_ref, v_ref, ot_ref, lse_ref, wo_ref, dh_ref, at_ref, cos_ref, sin_ref, _, dw_ref,
                       dot_s, delta_s, dq_s, dk_s, dv_s, *, scale):
    t = q_ref.shape[0]
    heads = q_ref.shape[1] // HEAD
    e = scale * LOG2E
    col = lambda i: slice(i * HEAD, i * HEAD + HEAD)
    dot_s[...] = _dot(wo_ref[0], dh_ref[...], 1, 1).astype(BF16)
    dw_ref[3] = _dot(ot_ref[...], dh_ref[...]).astype(BF16)
    for i in range(heads):
        delta_s[i : i + 1, :] = jnp.sum(dot_s[col(i), :].astype(F32) * ot_ref[col(i), :].astype(F32), axis=0, keepdims=True)
    dk_s[...] = jnp.zeros_like(dk_s)
    dv_s[...] = jnp.zeros_like(dv_s)
    dq_s[...] = jnp.zeros_like(dq_s)
    gap = lax.broadcasted_iota(jnp.int32, (BKB, BQB), 1) - lax.broadcasted_iota(jnp.int32, (BKB, BQB), 0)

    for a in range(0, t, BQB):
        queries = slice(a, a + BQB)
        for j in range(0, a + BQB, BKB):
            keys = slice(j, j + BKB)
            masked = j + BKB > a
            scores = [_dot(k_ref[keys, col(i)], q_ref[queries, col(i)], 1, 1) for i in range(heads)]
            dps = [_dot(v_ref[keys, col(i)], dot_s[col(i), queries]) for i in range(heads)]
            for i in range(heads):
                p = jnp.exp2(scores[i] * e - lse_ref[i : i + 1, queries])
                if masked:
                    p = jnp.where(gap >= j - a, p, 0.0)
                ds = (p * (dps[i] - delta_s[i : i + 1, queries])).astype(BF16)
                dv_s[keys, col(i)] += _dot(p.astype(BF16), dot_s[col(i), queries], 1, 1)
                dk_s[keys, col(i)] += _dot(ds, q_ref[queries, col(i)])
                dq_s[col(i), queries] += _dot(k_ref[keys, col(i)].T, ds)

    cos, sin = cos_ref[...], sin_ref[...]
    dw_ref[2] = _dot(at_ref[...], dv_s[...].astype(BF16)).astype(BF16)

    def turned_back(one):
        one = (one * scale).astype(BF16).astype(F32)
        return (one * cos - pltpu.roll(one, QUARTER, 1) * sin).astype(BF16)

    dk = jnp.concatenate([turned_back(dk_s[:, col(i)]) for i in range(heads)], axis=1)
    dw_ref[1] = _dot(at_ref[...], dk).astype(BF16)
    dq = jnp.concatenate([turned_back(dq_s[col(i), :].T) for i in range(heads)], axis=1)
    dw_ref[0] = _dot(at_ref[...], dq).astype(BF16)


def attend_bwd(q, k, v, ot, lse, wo, dh, at, cos, sin, dw):
    t = q.shape[0]
    whole = lambda a: pl.BlockSpec(a.shape, lambda i: (0,) * a.ndim)
    cols = pl.BlockSpec((t, D), lambda i: (0, i))
    vm = pltpu.VMEM
    lse = lse.reshape(4, 4, t)
    return pl.pallas_call(
        functools.partial(_attend_bwd_kernel, scale=HEAD**-0.5), grid=(4,),
        in_specs=[cols, cols, cols, pl.BlockSpec((D, t), lambda i: (i, 0)), pl.BlockSpec((None, 4, t), lambda i: (i, 0, 0)),
                  pl.BlockSpec((1, D, D), lambda i: (0, i, 0)), whole(dh), whole(at), whole(cos), whole(sin), pl.BlockSpec(memory_space=pl.ANY)],
        out_specs=pl.BlockSpec((4, D, D), lambda i: (LARGE // 4 + i, 0, 0)), out_shape=jax.ShapeDtypeStruct(dw.shape, BF16),
        input_output_aliases={10: 0},
        scratch_shapes=[vm((D, t), BF16), vm((4, t), F32), vm((D, t), F32), vm((t, D), F32), vm((t, D), F32)],
        compiler_params=_params(ANY), cost_estimate=_cost(3e10, 3e7, 1e7),
    )(q, k, v, ot, lse, wo, dh, at, cos, sin, dw)


MESH = pl.DeviceIdType.MESH
STRIDE = (EIGHTH, 8, 2)
LAG = 2
DEEP, SLOTS = 9, 5


def _reduce_kernel(nch, g_ref, out_ref, sum_ref, loc, rd, s1, r1, s2, r2, p1, s3, r3, s4, r4, p2, s5, r5, fin, ebuf, acc,
                   lsem, dsem, ssem, rsem, esem):
    me = lax.axis_index("dp")
    core = lax.rem(me, 2)
    pos = [lax.rem(lax.div(me, s), 4) for s in STRIDE]
    partner = me + 1 - 2 * core

    def peer(d, o):
        return me + (lax.rem(pos[d] + o, 4) - pos[d]) * STRIDE[d]

    barrier = pltpu.get_barrier_semaphore()
    for dev in [partner] + [peer(d, o) for d in range(3) for o in (1, 2, 3)]:
        pl.semaphore_signal(barrier, inc=1, device_id={"dp": dev}, device_id_type=MESH)
    pl.semaphore_wait(barrier, 10)

    acc[...] = jnp.zeros_like(acc)
    nt = -(-nch // 3)

    def send(src, dst, kind, slot, dev):
        return pltpu.make_async_remote_copy(src_ref=src, dst_ref=dst, send_sem=ssem.at[kind, slot], recv_sem=rsem.at[kind, slot],
                                            device_id={"dp": dev}, device_id_type=MESH)

    def stages(j):
        d1, d2, d3 = j, (j + 1) % 3, (j + 2) % 3
        q1, q2, q3 = pos[d1], pos[d2], pos[d3]
        right1, left1 = peer(d1, 1), peer(d1, 3)
        right2, left2 = peer(d2, 1), peer(d2, 3)
        at = lambda q, o: lax.rem(q + o, 4)
        rows = lambda start, n: pl.ds(pl.multiple_of(start, PIECE), n)
        lanes = lambda start, n: pl.ds(pl.multiple_of(start, HEAD), n)
        base = core * HALF
        row1 = base + q1 * QUARTER
        row2 = row1 + q2 * PIECE
        sl = lambda T: lax.rem(T, SLOTS) * 3 + j
        big = lambda T: lax.rem(T, DEEP) * 3 + j

        def copies(k, T):
            c, s, b = 3 * T + j, sl(T), big(T)
            if k == 0:
                return [pltpu.make_async_copy(g_ref.at[c, rows(base, HALF), :], loc.at[b], lsem.at[s]),
                        send(g_ref.at[c, rows(HALF - base, HALF), :], rd.at[b], 0, s, partner)]
            if k == 1:
                return [send(s1.at[s, 0], r1.at[s, 0], 1, s, right1), send(s1.at[s, 1], r1.at[s, 1], 2, s, left1)]
            if k == 2:
                return [send(s2.at[s, 0], r2.at[s, 0], 3, s, right1), send(s2.at[s, 1], r2.at[s, 1], 4, s, left1)]
            if k == 3:
                return [send(s3.at[s, 0], r3.at[s, 0], 5, s, right2), send(s3.at[s, 1], r3.at[s, 1], 6, s, left2)]
            if k == 4:
                return [send(s4.at[s, 0], r4.at[s, 0], 7, s, right2), send(s4.at[s, 1], r4.at[s, 1], 8, s, left2)]
            if k == 5:
                return [send(s5.at[s, o - 1], r5.at[s, o - 1], 8 + o, s, peer(d3, o)) for o in (1, 2, 3)]
            if k == 6:
                home = out_ref.at[c, rows(row2, PIECE), lanes(q3 * HEAD, HEAD)]
                return [pltpu.make_async_copy(fin.at[s], home, dsem.at[s])] + [
                    send(fin.at[s], home, 11 + o, s, peer(d3, o)) for o in (1, 2, 3)]
            if k == 7:
                mine = out_ref.at[c, rows(row2, PIECE), :]
                return [send(mine, mine, 15, s, right2), send(mine, mine, PIECE, s, left2)]
            if k == 8:
                a = out_ref.at[c, rows(row1 + at(q2, 3) * PIECE, PIECE), pl.ds(0, HALF)]
                z = out_ref.at[c, rows(row1 + at(q2, 1) * PIECE, PIECE), pl.ds(HALF, HALF)]
                return [send(a, a, 17, s, right2), send(z, z, 18, s, left2)]
            if k == 9:
                mine = out_ref.at[c, rows(row1, QUARTER), :]
                return [send(mine, mine, 19, s, right1), send(mine, mine, 20, s, left1)]
            if k == 10:
                a = out_ref.at[c, rows(base + at(q1, 3) * QUARTER, EIGHTH), :]
                z = out_ref.at[c, rows(base + at(q1, 1) * QUARTER + EIGHTH, EIGHTH), :]
                return [send(a, a, 21, s, right1), send(z, z, 22, s, left1)]
            if k == 11:
                mine = out_ref.at[c, rows(base, HALF), :]
                return [send(mine, mine, 23, s, partner)]
            return []

        def both(T, start, n):
            here = (big(T), rows(start, n))
            return loc[here].astype(F32) + rd[here].astype(F32)

        def work(k, T):
            s = sl(T)
            if k == 1:
                far = at(q1, 2) * QUARTER
                s1[s, 0] = both(T, far, EIGHTH).astype(BF16)
                s1[s, 1] = both(T, far + EIGHTH, EIGHTH).astype(BF16)
            if k == 2:
                a, z = at(q1, 1) * QUARTER, at(q1, 3) * QUARTER
                s2[s, 0, :EIGHTH] = (both(T, a, EIGHTH) + r1[s, 0].astype(F32)).astype(BF16)
                s2[s, 0, EIGHTH:] = both(T, a + EIGHTH, EIGHTH).astype(BF16)
                s2[s, 1, :EIGHTH] = both(T, z, EIGHTH).astype(BF16)
                s2[s, 1, EIGHTH:] = (both(T, z + EIGHTH, EIGHTH) + r1[s, 1].astype(F32)).astype(BF16)
            if k == 3:
                p1[s] = both(T, q1 * QUARTER, QUARTER) + r2[s, 0].astype(F32) + r2[s, 1].astype(F32)
                far = p1[s, rows(at(q2, 2) * PIECE, PIECE), :].astype(BF16)
                s3[s, 0] = far[:, :HALF]
                s3[s, 1] = far[:, HALF:]
            if k == 4:
                a, z = p1[s, rows(at(q2, 1) * PIECE, PIECE), :], p1[s, rows(at(q2, 3) * PIECE, PIECE), :]
                s4[s, 0, :, :HALF] = (a[:, :HALF] + r3[s, 0].astype(F32)).astype(BF16)
                s4[s, 0, :, HALF:] = a[:, HALF:].astype(BF16)
                s4[s, 1, :, :HALF] = z[:, :HALF].astype(BF16)
                s4[s, 1, :, HALF:] = (z[:, HALF:] + r3[s, 1].astype(F32)).astype(BF16)
            if k == 5:
                p2[s] = p1[s, rows(q2 * PIECE, PIECE), :] + r4[s, 0].astype(F32) + r4[s, 1].astype(F32)
                for o in (1, 2, 3):
                    s5[s, o - 1] = p2[s, :, lanes(at(q3, o) * HEAD, HEAD)].astype(BF16)
            if k == 6:
                total = p2[s, :, lanes(q3 * HEAD, HEAD)]
                for o in (1, 2, 3):
                    total += r5[s, o - 1].astype(F32)
                total = total.astype(BF16)
                fin[s] = total
                acc[...] += total.astype(F32) * total.astype(F32)

        return copies, work

    streams = [stages(j) for j in range(3)]

    def one(t, k):
        T = t - LAG * k
        for j, (copies, work) in enumerate(streams):

            @pl.when((T >= 0) & (3 * T + j < nch))
            def _():
                if k > 0:
                    for copy in copies(k - 1, T):
                        copy.wait()
                work(k, T)
                for copy in copies(k, T):
                    copy.start()

    exchanged = nt + LAG * 6

    def exchange(k):
        def hops(k):
            if k == 3:
                return [(0, core, partner)]
            return [(o - 1, pos[k], peer(k, o)) for o in (1, 2, 3)]

        def moves(k):
            return [pltpu.make_async_remote_copy(src_ref=ebuf.at[k, place], dst_ref=ebuf.at[k, place], send_sem=esem.at[0, k, n],
                                                 recv_sem=esem.at[1, k, n], device_id={"dp": dev}, device_id_type=MESH)
                    for n, place, dev in hops(k)]

        if k > 0:
            for copy in moves(k - 1):
                copy.wait()
            total = ebuf[k - 1, 0] + ebuf[k - 1, 1]
            if k < 4:
                total = total + ebuf[k - 1, 2] + ebuf[k - 1, 3]
        else:
            total = acc[...]
        if k == 4:
            sum_ref[...] = total
        else:
            ebuf[k, hops(k)[0][1]] = total
            for copy in moves(k):
                copy.start()

    def tick(t, _):
        for k in range(12, -1, -1):
            one(t, k)
        for k in range(5):
            pl.when(t == exchanged + 2 * k)(functools.partial(exchange, k))

    lax.fori_loop(0, nt + LAG * 12, tick, None)


def all_reduce(g):
    nch = g.shape[0]
    deep, n = 3 * DEEP, 3 * SLOTS
    vm = pltpu.VMEM
    out, total = pl.pallas_call(
        functools.partial(_reduce_kernel, nch),
        out_shape=[jax.ShapeDtypeStruct(g.shape, BF16), jax.ShapeDtypeStruct((PIECE, HEAD), F32)],
        in_specs=[pl.BlockSpec(memory_space=pl.ANY)],
        out_specs=[pl.BlockSpec(memory_space=pl.ANY), pl.BlockSpec(memory_space=pltpu.VMEM)],
        scratch_shapes=[
            vm((deep, HALF, D), BF16), vm((deep, HALF, D), BF16),
            vm((n, 2, EIGHTH, D), BF16), vm((n, 2, EIGHTH, D), BF16),
            vm((n, 2, QUARTER, D), BF16), vm((n, 2, QUARTER, D), BF16),
            vm((n, QUARTER, D), F32),
            vm((n, 2, PIECE, HALF), BF16), vm((n, 2, PIECE, HALF), BF16),
            vm((n, 2, PIECE, D), BF16), vm((n, 2, PIECE, D), BF16),
            vm((n, PIECE, D), F32),
            vm((n, 3, PIECE, HEAD), BF16), vm((n, 3, PIECE, HEAD), BF16),
            vm((n, PIECE, HEAD), BF16),
            vm((4, 4, PIECE, HEAD), F32), vm((PIECE, HEAD), F32),
            pltpu.SemaphoreType.DMA((n,)), pltpu.SemaphoreType.DMA((n,)),
            pltpu.SemaphoreType.DMA((24, n)), pltpu.SemaphoreType.DMA((24, n)), pltpu.SemaphoreType.DMA((2, 4, 3)),
        ],
        compiler_params=pltpu.CompilerParams(collective_id=0, has_side_effects=True, vmem_limit_bytes=56 * 2**20),
    )(g)
    return out, total


STEPS = 32


def _adamw_kernel(count, sum_ref, *refs):
    g, w, m, v, new_w, new_m, new_v = (refs[7 * i : 7 * i + 7] for i in range(7))
    i = pl.program_id(0)
    factor = jnp.minimum(1.0, 0.5 * lax.rsqrt(jnp.sum(sum_ref[...], keepdims=True) / count + 1e-30))

    def update(n):
        gradient = g[n][0].astype(F32) * factor
        if n == 6:
            gradient = gradient.T
        mean = 0.9 * m[n][0] + 0.1 * gradient
        square = 0.95 * v[n][0] + 0.05 * gradient * gradient
        weight = w[n][0].astype(F32)
        step = mean * lax.rsqrt(square + 1e-8) + 0.1 * weight
        new_w[n][0] = (weight - 0.02 * step).astype(BF16)
        new_m[n][0] = mean
        new_v[n][0] = square

    @pl.when(i < STEPS)
    def _():
        for n in (4, 5, 6):
            update(n)

    @pl.when(i >= STEPS)
    def _():
        for n in (0, 1, 2, 3):
            update(n)


def adamw(g, total, weights, m, v):
    def step(n):
        return lambda i: jnp.minimum(i, STEPS - 1) if n >= 4 else jnp.maximum(i - STEPS, 0)

    def own(n):
        at = step(n)
        if n in (3, 6):
            return pl.BlockSpec((1, HALF, D), lambda i: (0, at(i), 0))
        return pl.BlockSpec((1, HALF, D), lambda i: (0, lax.rem(at(i), 2), lax.div(at(i), 2)))

    def part(n):
        at = step(n)
        chunk = lambda i: (3 * lax.div(at(i), 2) + n - 4) if n >= 4 else (LARGE + 4 * lax.div(at(i), 2) + n)
        if n == 6:
            return pl.BlockSpec((1, D, HALF), lambda i: (chunk(i), 0, lax.rem(at(i), 2)))
        return pl.BlockSpec((1, HALF, D), lambda i: (chunk(i), lax.rem(at(i), 2), 0))

    owns = [own(n) for n in range(7)]
    shapes = [jax.ShapeDtypeStruct(w.shape, BF16) for w in weights] + [jax.ShapeDtypeStruct(w.shape, F32) for w in weights] * 2
    return pl.pallas_call(
        functools.partial(_adamw_kernel, float(sum(w.size for w in weights))),
        grid=(STEPS + 8,),
        in_specs=[pl.BlockSpec((PIECE, HEAD), lambda i: (0, 0))] + [part(n) for n in range(7)] + owns * 3,
        out_specs=owns * 3,
        out_shape=shapes,
        compiler_params=_params(ANY),
        cost_estimate=_cost(2.5e8, 3.7e8, 1.7e7),
    )(total, *([g] * 7), *weights, *m, *v)


def solution(mesh):
    def step(x, dy, *arrays):
        weights, m, v = (arrays[i : i + 7] for i in (0, 7, 14))
        wq, wk, wv, wo, w_gate, w_up, w_down = weights
        x, dy = x[0], dy[0]
        cos, sin = tables(x.shape[0])
        q, k, value, at = qkv(x, wq, wk, wv, cos, sin)
        o, ot, lse = attend(q, k, value)
        dw, dh = mlp(x, o, wo, dy, w_gate, w_up, w_down)
        dw = attend_bwd(q, k, value, ot, lse, wo, dh, at, cos, sin, dw)
        summed, total = all_reduce(dw)
        return tuple(adamw(summed, total, weights, m, v))

    states, all_of = P(("rep", "dp"), None, None), P(None, None, None)
    return jax.shard_map(
        step,
        mesh=mesh,
        in_specs=(states, states) + (all_of,) * 21,
        out_specs=(P("rep", None, None),) * 21,
        check_vma=False,
    )
```

```python
import functools

import jax
import jax.numpy as jnp
from jax import lax
from jax.experimental import pallas as pl
from jax.experimental.pallas import tpu as pltpu
from jax.sharding import PartitionSpec as P

F32, BF16 = jnp.float32, jnp.bfloat16
NEG = -1e30
HIDDEN = 2 * NEG
LOG2E = 1.4426950408889634
D, HALF, HEAD, QUARTER, EIGHTH, PIECE = 512, 256, 128, 64, 32, 16
THETA = 10000
VMEM = 63 * 2**20
ANY = "arbitrary"
MESH = pl.DeviceIdType.MESH
SCALE = HEAD**-0.5
E2 = SCALE * LOG2E


def _dot(a, b, ca=1, cb=0):
    return lax.dot_general(a, b, (((ca,), (cb,)), ((), ())), preferred_element_type=F32)


def _params(**more):
    return pltpu.CompilerParams(dimension_semantics=(ANY,), vmem_limit_bytes=VMEM, **more)


def _cost(flops, nbytes, exps=0):
    return pl.CostEstimate(flops=int(flops), bytes_accessed=int(nbytes), transcendentals=int(exps))


def _whole(*shape):
    return pl.BlockSpec(shape, lambda i: (0,) * len(shape), pipeline_mode=pl.Buffered(1))


def _col(i):
    return slice(i * HEAD, i * HEAD + HEAD)


def _norm_scale(wide):
    return lax.rsqrt(jnp.mean(wide * wide, -1, keepdims=True) + 1e-6)


def tables(tokens):
    half = HEAD // 2
    angle = jnp.arange(tokens, dtype=F32)[:, None] * THETA ** (-jnp.arange(half, dtype=F32) / half)
    cos, sin = jnp.cos(angle), jnp.sin(angle)
    return jnp.concatenate([cos, cos], 1), jnp.concatenate([-sin, sin], 1)


def _qkv_kernel(x_ref, wq_ref, wk_ref, wv_ref, cos_ref, sin_ref, q_ref, k_ref, v_ref, at_ref, a_s):
    t = x_ref.shape[0]

    @pl.when(pl.program_id(0) == 0)
    def _():
        wide = x_ref[...].astype(F32)
        a_s[...] = (wide * _norm_scale(wide)).astype(BF16)
        at_ref[...] = a_s[...].T

    for r in range(0, t, HALF):
        here = slice(r, r + HALF)
        for w, out in ((wq_ref, q_ref), (wk_ref, k_ref)):
            whole = _dot(a_s[here], w[0]).astype(BF16).astype(F32)
            for i in range(D // HEAD):
                one = whole[:, _col(i)]
                out[here, _col(i)] = (one * cos_ref[here] + pltpu.roll(one, HEAD // 2, 1) * sin_ref[here]).astype(BF16)
        v_ref[here] = _dot(a_s[here], wv_ref[0]).astype(BF16)


def qkv(x, wq, wk, wv, cos, sin):
    t, width = x.shape[0], wq.shape[2]
    cols = pl.BlockSpec((t, D), lambda i: (0, i))
    w = pl.BlockSpec((1, D, D), lambda i: (0, 0, i))
    out = jax.ShapeDtypeStruct((t, width), BF16)
    return pl.pallas_call(
        _qkv_kernel, grid=(width // D,), in_specs=[_whole(t, D), w, w, w, _whole(t, HEAD), _whole(t, HEAD)],
        out_specs=[cols, cols, cols, pl.BlockSpec((D, t), lambda i: (0, 0))], out_shape=[out, out, out, jax.ShapeDtypeStruct((D, t), BF16)],
        scratch_shapes=[pltpu.VMEM((t, D), BF16)], compiler_params=_params(), cost_estimate=_cost(6.4e9, 2e7),
    )(x, wq, wk, wv, cos, sin)


BQ = HALF


def _attend_kernel(q_ref, k_ref, v_ref, x_ref, dy_ref, wo_ref, ot_ref, lse_ref, h_ref, b_ref, bt_ref, dyt_ref, top_s, mix_s, o_s):
    iq = pl.program_id(0)
    heads = q_ref.shape[1] // HEAD
    top_s[...] = jnp.full_like(top_s, NEG)
    mix_s[...] = jnp.zeros_like(mix_s)
    ones = jnp.ones((8, BQ), BF16)
    hidden = lax.broadcasted_iota(jnp.int32, (BQ, BQ), 0) > lax.broadcasted_iota(jnp.int32, (BQ, BQ), 1)

    def block(j, masked):
        here = pl.ds(pl.multiple_of(j * BQ, BQ), BQ)
        scores = [_dot(k_ref[here, _col(i)], q_ref[:, _col(i)], 1, 1) for i in range(heads)]
        weights, keeps = [], []
        for i, s in enumerate(scores):
            if masked:
                s = jnp.where(hidden, HIDDEN, s)
            old = top_s[i : i + 1, :]
            top = jnp.maximum(old, s.max(axis=0, keepdims=True))
            top_s[i : i + 1, :] = top
            weights.append(jnp.exp2((s - top) * E2).astype(BF16))
            keeps.append(jnp.exp2((old - top) * E2))
        for i, (p, keep) in enumerate(zip(weights, keeps)):
            values = jnp.concatenate([v_ref[here, _col(i)].T, ones], axis=0)
            mix_s[i] = mix_s[i] * keep + _dot(values, p)

    lax.fori_loop(0, iq, lambda j, _: block(j, False), None)
    block(iq, True)
    for i in range(heads):
        total = mix_s[i, HEAD : HEAD + 1, :]
        out = (mix_s[i, :HEAD, :] * (1 / total)).astype(BF16)
        ot_ref[_col(i), :] = out
        o_s[:, _col(i)] = out.T
        lse_ref[i : i + 1, :] = top_s[i : i + 1, :] * E2 + jnp.log2(total)
    h = (x_ref[...].astype(F32) + _dot(o_s[...], wo_ref[0]).astype(BF16).astype(F32)).astype(BF16)
    h_ref[...] = h
    wide = h.astype(F32)
    b = (wide * _norm_scale(wide)).astype(BF16)
    b_ref[...] = b
    bt_ref[...] = b.T
    dyt_ref[...] = dy_ref[...].T


def attend(q, k, v, x, dy, wo):
    t, width = q.shape
    heads = width // HEAD
    rows = lambda n: pl.BlockSpec((BQ, n), lambda i: (i, 0))
    cols = lambda n: pl.BlockSpec((n, BQ), lambda i: (0, i))
    shape = jax.ShapeDtypeStruct
    return pl.pallas_call(
        _attend_kernel, grid=(t // BQ,), in_specs=[rows(width), _whole(t, width), _whole(t, width), rows(D), rows(D), _whole(1, width, D)],
        out_specs=[cols(width), cols(heads), rows(D), rows(D), cols(D), cols(D)],
        out_shape=[shape((width, t), BF16), shape((heads, t), F32), shape((t, D), BF16), shape((t, D), BF16), shape((D, t), BF16), shape((D, t), BF16)],
        scratch_shapes=[pltpu.VMEM((heads, BQ), F32), pltpu.VMEM((heads, HEAD + 8, BQ), F32), pltpu.VMEM((BQ, width), BF16)],
        compiler_params=_params(), cost_estimate=_cost(1.2e10, 2e7, 1e7),
    )(q, k, v, x, dy, wo)


STRIDE = (32, 8, 2)
MLP, GROUPS, SUBS = 16, 4, 3
STEPS = MLP + GROUPS * SUBS
CHUNKS = 32
STAGES = 13
SMALL = MLP + 2 * SUBS
LAST = SMALL + 2 * SUBS
SLOTS = 9


def _reducer(grad, rd, s1, r1, s2, r2, p1, s3, r3, s4, r4, p2, s5, r5, fin, ebuf, acc, dsem, ssem, rsem, esem, out_ref, sum_ref):
    me = lax.axis_index("dp")
    core = lax.rem(me, 2)
    pos = [lax.rem(lax.div(me, s), 4) for s in STRIDE]
    partner = me + 1 - 2 * core

    def peer(d, o):
        return me + (lax.rem(pos[d] + o, 4) - pos[d]) * STRIDE[d]

    def begin():
        barrier = pltpu.get_barrier_semaphore()
        for dev in [partner] + [peer(d, o) for d in range(3) for o in (1, 2, 3)]:
            pl.semaphore_signal(barrier, inc=1, device_id={"dp": dev}, device_id_type=MESH)
        pl.semaphore_wait(barrier, 10)
        acc[...] = jnp.zeros_like(acc)

    rows = lambda start, n: pl.ds(pl.multiple_of(start, PIECE), n)
    lanes = lambda start, n: pl.ds(pl.multiple_of(start, HEAD), n)
    at = lambda q, o: lax.rem(q + o, 4)
    base = core * HALF

    def send(src, dst, kind, s, dev):
        return pltpu.make_async_remote_copy(src_ref=src, dst_ref=dst, send_sem=ssem.at[kind, s], recv_sem=rsem.at[kind, s],
                                            device_id={"dp": dev}, device_id_type=MESH)

    def stream(j):
        d1, d2, d3 = j, (j + 1) % 3, (j + 2) % 3
        q1, q2, q3 = pos[d1], pos[d2], pos[d3]
        row1 = base + q1 * QUARTER
        row2 = row1 + q2 * PIECE

        def copies(k, c):
            s = lax.rem(c, SLOTS)
            right1, left1, right2, left2 = peer(d1, 1), peer(d1, 3), peer(d2, 1), peer(d2, 3)
            home = lambda row, n, lane=pl.ds(0, D): out_ref.at[pl.ds(2 * c, 2), rows(row, n), lane]
            if k == 0:
                return [send(grad.at[s, :, rows(HALF - base, HALF), :], rd.at[s], 0, s, partner)]
            if k in (1, 2, 3, 4):
                src, dst = ((s1, r1), (s2, r2), (s3, r3), (s4, r4))[k - 1]
                right, left = (right1, left1) if k < 3 else (right2, left2)
                return [send(src.at[s, 0], dst.at[s, 0], 2 * k - 1, s, right), send(src.at[s, 1], dst.at[s, 1], 2 * k, s, left)]
            if k == 5:
                return [send(s5.at[s, o - 1], r5.at[s, o - 1], 8 + o, s, peer(d3, o)) for o in (1, 2, 3)]
            if k == 6:
                mine = home(row2, PIECE, lanes(q3 * HEAD, HEAD))
                return [pltpu.make_async_copy(fin.at[s], mine, dsem.at[s])] + [send(fin.at[s], mine, 11 + o, s, peer(d3, o)) for o in (1, 2, 3)]
            if k == 7:
                mine = home(row2, PIECE)
                return [send(mine, mine, 15, s, right2), send(mine, mine, 16, s, left2)]
            if k == 8:
                a = home(row1 + at(q2, 3) * PIECE, PIECE, pl.ds(0, HALF))
                z = home(row1 + at(q2, 1) * PIECE, PIECE, pl.ds(HALF, HALF))
                return [send(a, a, 17, s, right2), send(z, z, 18, s, left2)]
            if k == 9:
                mine = home(row1, QUARTER)
                return [send(mine, mine, 19, s, right1), send(mine, mine, 20, s, left1)]
            if k == 10:
                a = home(base + at(q1, 3) * QUARTER, EIGHTH)
                z = home(base + at(q1, 1) * QUARTER + EIGHTH, EIGHTH)
                return [send(a, a, 21, s, right1), send(z, z, 22, s, left1)]
            if k == 11:
                mine = home(base, HALF)
                return [send(mine, mine, 23, s, partner)]
            return []

        def work(k, c):
            s = lax.rem(c, SLOTS)

            def both(start, n):
                return grad[s, :, rows(base + start, n), :].astype(F32) + rd[s, :, rows(start, n), :].astype(F32)

            if k == 1:
                far = at(q1, 2) * QUARTER
                s1[s, 0] = both(far, EIGHTH).astype(BF16)
                s1[s, 1] = both(far + EIGHTH, EIGHTH).astype(BF16)
            if k == 2:
                a, z = at(q1, 1) * QUARTER, at(q1, 3) * QUARTER
                s2[s, 0, :, :EIGHTH] = (both(a, EIGHTH) + r1[s, 0].astype(F32)).astype(BF16)
                s2[s, 0, :, EIGHTH:] = both(a + EIGHTH, EIGHTH).astype(BF16)
                s2[s, 1, :, :EIGHTH] = both(z, EIGHTH).astype(BF16)
                s2[s, 1, :, EIGHTH:] = (both(z + EIGHTH, EIGHTH) + r1[s, 1].astype(F32)).astype(BF16)
            if k == 3:
                p1[s] = both(q1 * QUARTER, QUARTER) + r2[s, 0].astype(F32) + r2[s, 1].astype(F32)
                far = p1[s, :, rows(at(q2, 2) * PIECE, PIECE), :].astype(BF16)
                s3[s, 0] = far[:, :, :HALF]
                s3[s, 1] = far[:, :, HALF:]
            if k == 4:
                a, z = p1[s, :, rows(at(q2, 1) * PIECE, PIECE), :], p1[s, :, rows(at(q2, 3) * PIECE, PIECE), :]
                s4[s, 0, :, :, :HALF] = (a[:, :, :HALF] + r3[s, 0].astype(F32)).astype(BF16)
                s4[s, 0, :, :, HALF:] = a[:, :, HALF:].astype(BF16)
                s4[s, 1, :, :, :HALF] = z[:, :, :HALF].astype(BF16)
                s4[s, 1, :, :, HALF:] = (z[:, :, HALF:] + r3[s, 1].astype(F32)).astype(BF16)
            if k == 5:
                p2[s] = p1[s, :, rows(q2 * PIECE, PIECE), :] + r4[s, 0].astype(F32) + r4[s, 1].astype(F32)
                for o in (1, 2, 3):
                    s5[s, o - 1] = p2[s, :, :, lanes(at(q3, o) * HEAD, HEAD)].astype(BF16)
            if k == 6:
                total = p2[s, :, :, lanes(q3 * HEAD, HEAD)]
                for o in (1, 2, 3):
                    total += r5[s, o - 1].astype(F32)
                total = total.astype(BF16)
                fin[s] = total
                square = total.astype(F32) * total.astype(F32)
                acc[...] += square[0] + square[1]

        return copies, work

    streams = [stream(j) for j in range(3)]

    def stage(t, k):
        u = t - k
        small = lax.div(u - SMALL, SUBS)
        large = lax.div(u - 2, 2)
        of_large = (u >= 2) & (u <= MLP) & (large * 2 == u - 2)
        of_small = (u >= SMALL) & (u <= LAST) & (small * SUBS == u - SMALL)
        triple = jnp.where(of_large, large, MLP // 2 + small)
        for j, (copies, work) in enumerate(streams):
            c = 3 * triple + j

            @pl.when((of_large | of_small) & (c < CHUNKS))
            def _():
                if k > 0:
                    for copy in copies(k - 1, c):
                        copy.wait()
                work(k, c)
                for copy in copies(k, c):
                    copy.start()

    def hops(k):
        if k == 3:
            return [(0, core, partner)]
        return [(o - 1, pos[k], peer(k, o)) for o in (1, 2, 3)]

    def moves(k):
        return [pltpu.make_async_remote_copy(src_ref=ebuf.at[k, place], dst_ref=ebuf.at[k, place], send_sem=esem.at[0, k, n],
                                             recv_sem=esem.at[1, k, n], device_id={"dp": dev}, device_id_type=MESH)
                for n, place, dev in hops(k)]

    def exchange(k):
        if k > 0:
            for copy in moves(k - 1):
                copy.wait()
            total = ebuf[k - 1, 0] + ebuf[k - 1, 1]
            if k < 4:
                total = total + ebuf[k - 1, 2] + ebuf[k - 1, 3]
        else:
            total = acc[...]
        if k == 4:
            sum_ref[...] = total
        else:
            ebuf[k, hops(k)[0][1]] = total
            for copy in moves(k):
                copy.start()

    def tick(t):
        for k in range(STAGES - 1, -1, -1):
            stage(t, k)

    def finish():
        def late(t, _):
            tick(t)
            for k in range(5):
                pl.when(t == LAST + 7 + k)(functools.partial(exchange, k))

        lax.fori_loop(STEPS, LAST + STAGES, late, None)

    return begin, tick, finish


def _mlp_step(i, b_ref, bt_ref, dy_ref, dyt_ref, wg_ref, wu_ref, wd_ref, h_ref, grad, db_s, dh_s, hid_s, dg_s, du_s):
    t = b_ref.shape[0]
    parts = [slice(r, r + HALF) for r in range(0, t, HALF)]

    @pl.when(i == 0)
    def _():
        db_s[...] = jnp.zeros_like(db_s)

    wg, wu, wd = wg_ref[0], wu_ref[0], wd_ref[0]
    for here in parts:
        gate, up = _dot(b_ref[here], wg), _dot(b_ref[here], wu)
        dh = _dot(dy_ref[here], wd, 1, 1).astype(BF16).astype(F32)
        sig = 0.5 * jnp.tanh(0.5 * gate) + 0.5
        act = gate * sig
        hid_s[here] = (act * up).astype(BF16)
        du_s[here] = (dh * act).astype(BF16)
        dg_s[here] = (dh * up * (sig + act * (1 - sig))).astype(BF16)
    for here in parts:
        db_s[here] += _dot(dg_s[here], wg, 1, 1) + _dot(du_s[here], wu, 1, 1)
    first, n = 3 * lax.div(i, 2), lax.rem(i, 2)
    grad[lax.rem(first, SLOTS), n] = _dot(bt_ref[...], dg_s[...]).astype(BF16)
    grad[lax.rem(first + 1, SLOTS), n] = _dot(bt_ref[...], du_s[...]).astype(BF16)
    grad[lax.rem(first + 2, SLOTS), n] = _dot(dyt_ref[...], hid_s[...]).astype(BF16)

    @pl.when(i == MLP - 1)
    def _():
        for here in parts:
            db = db_s[here].astype(BF16).astype(F32)
            wide = h_ref[here].astype(F32)
            scale = _norm_scale(wide)
            inner = jnp.mean(db * wide, -1, keepdims=True)
            dh_s[here] = (dy_ref[here].astype(F32) + (db * scale - wide * (scale * scale * scale * inner))).astype(BF16)


def _attend_step(g, sub, q_ref, k_ref, v_ref, ot_ref, lse_ref, wo_ref, at_ref, cos_ref, sin_ref, grad, dh_s, dot_s, delta_s, dq_s, dk_s, dv_s):
    t = q_ref.shape[0]
    heads = range(q_ref.shape[1] // HEAD)
    half = t // 2
    gap = lax.broadcasted_iota(jnp.int32, (BQ, half), 1) - lax.broadcasted_iota(jnp.int32, (BQ, half), 0)
    first = lax.rem(CHUNKS - 2 * GROUPS + 2 * g, SLOTS)
    second = lax.rem(first + 1, SLOTS)

    def block(a, j):
        queries, keys = slice(a, a + half), slice(j, j + BQ)
        scores = [_dot(k_ref[keys, _col(i)], q_ref[queries, _col(i)], 1, 1) for i in heads]
        dps = [_dot(v_ref[keys, _col(i)], dot_s[_col(i), queries]) for i in heads]
        for i in heads:
            p = jnp.exp2(scores[i] * E2 - lse_ref[i : i + 1, queries])
            if j + BQ > a:
                p = jnp.where(gap >= j - a, p, 0.0)
            ds = (p * (dps[i] - delta_s[i : i + 1, queries])).astype(BF16)
            dv_s[keys, _col(i)] += _dot(p.astype(BF16), dot_s[_col(i), queries], 1, 1)
            dk_s[keys, _col(i)] += _dot(ds, q_ref[queries, _col(i)])
            dq_s[_col(i), queries] += _dot(k_ref[keys, _col(i)].T, ds)

    def turned_back(one):
        one = (one * SCALE).astype(BF16).astype(F32)
        return (one * cos_ref[...] - pltpu.roll(one, HEAD // 2, 1) * sin_ref[...]).astype(BF16)

    @pl.when(sub == 0)
    def _():
        dot_s[...] = _dot(wo_ref[0], dh_s[...], 1, 1).astype(BF16)
        grad[second, 1] = _dot(ot_ref[...], dh_s[...]).astype(BF16)
        for i in heads:
            delta_s[i : i + 1, :] = jnp.sum(dot_s[_col(i), :].astype(F32) * ot_ref[_col(i), :].astype(F32), axis=0, keepdims=True)
        for total in (dq_s, dk_s, dv_s):
            total[...] = jnp.zeros_like(total)
        for j in range(0, half, BQ):
            block(0, j)

    @pl.when(sub == 1)
    def _():
        for j in range(0, half, BQ):
            block(half, j)

    @pl.when(sub == 2)
    def _():
        for j in range(half, t, BQ):
            block(half, j)
        grad[second, 0] = _dot(at_ref[...], dv_s[...].astype(BF16)).astype(BF16)
        dk = jnp.concatenate([turned_back(dk_s[:, _col(i)]) for i in heads], axis=1)
        grad[first, 1] = _dot(at_ref[...], dk).astype(BF16)
        dq = jnp.concatenate([turned_back(dq_s[_col(i), :].T) for i in heads], axis=1)
        grad[first, 0] = _dot(at_ref[...], dq).astype(BF16)


def _backward_kernel(b_ref, bt_ref, dy_ref, dyt_ref, wg_ref, wu_ref, wd_ref, h_ref, q_ref, k_ref, v_ref, ot_ref, lse_ref, wo_ref, at_ref, cos_ref,
                     sin_ref, out_ref, sum_ref, dh_s, hid_s, dg_s, du_s, dot_s, delta_s, dq_s, dk_s, dv_s, grad, *rest):
    p = pl.program_id(0)
    begin, tick, finish = _reducer(grad, *rest, out_ref, sum_ref)
    pl.when(p == 0)(begin)
    tick(p)

    @pl.when(p < MLP)
    def _():
        _mlp_step(p, b_ref, bt_ref, dy_ref, dyt_ref, wg_ref, wu_ref, wd_ref, h_ref, grad, dk_s, dh_s, hid_s, dg_s, du_s)

    @pl.when(p >= MLP)
    def _():
        _attend_step(lax.div(p - MLP, SUBS), lax.rem(p - MLP, SUBS), q_ref, k_ref, v_ref, ot_ref, lse_ref, wo_ref, at_ref, cos_ref, sin_ref, grad, dh_s,
                     dot_s, delta_s, dq_s, dk_s, dv_s)

    pl.when(p == STEPS - 1)(finish)


def backward(b, bt, dy, dyt, wg, wu, wd, h, q, k, v, ot, lse, wo, at, cos, sin):
    t = b.shape[0]
    large = lambda p: jnp.minimum(p, MLP - 1)
    group = lambda p: lax.div(jnp.clip(p - MLP, 0, GROUPS * SUBS - 1), SUBS)
    cols = pl.BlockSpec((1, D, D), lambda p: (0, 0, large(p)))
    heads = pl.BlockSpec((t, D), lambda p: (0, group(p)))
    vm, sem = pltpu.VMEM, pltpu.SemaphoreType.DMA
    two = lambda *shape: vm((SLOTS, 2, 2) + shape, BF16)
    three = vm((SLOTS, 3, 2, PIECE, HEAD), BF16)
    lse = lse.reshape(GROUPS, -1, t)
    return pl.pallas_call(
        _backward_kernel, grid=(STEPS,),
        in_specs=[_whole(t, D), _whole(D, t), _whole(t, D), _whole(D, t), cols, cols, pl.BlockSpec((1, D, D), lambda p: (0, large(p), 0)), _whole(t, D),
                  heads, heads, heads, pl.BlockSpec((D, t), lambda p: (group(p), 0)), pl.BlockSpec((None,) + lse.shape[1:], lambda p: (group(p), 0, 0)),
                  pl.BlockSpec((1, D, D), lambda p: (0, group(p), 0)), _whole(D, t), _whole(t, HEAD), _whole(t, HEAD)],
        out_specs=[pl.BlockSpec(memory_space=pl.ANY), pl.BlockSpec((PIECE, HEAD), lambda p: (0, 0))],
        out_shape=[jax.ShapeDtypeStruct((2 * CHUNKS, D, D), BF16), jax.ShapeDtypeStruct((PIECE, HEAD), F32)],
        scratch_shapes=[vm((t, D), BF16), vm((t, D), BF16), vm((t, D), BF16), vm((t, D), BF16), vm((D, t), BF16), vm((4, t), F32), vm((D, t), F32),
                        vm((t, D), F32), vm((t, D), F32), vm((SLOTS, 2, D, D), BF16), vm((SLOTS, 2, HALF, D), BF16), two(EIGHTH, D), two(EIGHTH, D),
                        two(QUARTER, D), two(QUARTER, D), vm((SLOTS, 2, QUARTER, D), F32), two(PIECE, HALF), two(PIECE, HALF), two(PIECE, D),
                        two(PIECE, D), vm((SLOTS, 2, PIECE, D), F32), three, three, vm((SLOTS, 2, PIECE, HEAD), BF16), vm((4, 4, PIECE, HEAD), F32),
                        vm((PIECE, HEAD), F32), sem((SLOTS,)), sem((24, SLOTS)), sem((24, SLOTS)), sem((2, 4, 3))],
        compiler_params=_params(collective_id=0, has_side_effects=True), cost_estimate=_cost(1.1e11, 1e8, 2e7),
    )(b, bt, dy, dyt, wg, wu, wd, h, q, k, v, ot, lse, wo, at, cos, sin)


def _adamw_kernel(count, sum_ref, *refs):
    g, w, m, v, new_w, new_m, new_v = (refs[7 * i : 7 * i + 7] for i in range(7))
    i = pl.program_id(0)
    factor = jnp.minimum(1.0, 0.5 * lax.rsqrt(jnp.sum(sum_ref[...], keepdims=True) / count + 1e-30))

    def update(n):
        gradient = g[n][0].astype(F32) * factor
        if n == 6:
            gradient = gradient.T
        mean = 0.9 * m[n][0] + 0.1 * gradient
        square = 0.95 * v[n][0] + 0.05 * gradient * gradient
        weight = w[n][0].astype(F32)
        step = mean * lax.rsqrt(square + 1e-8) + 0.1 * weight
        new_w[n][0] = (weight - 0.02 * step).astype(BF16)
        new_m[n][0] = mean
        new_v[n][0] = square

    @pl.when(i < MLP)
    def _():
        for n in (4, 5, 6):
            update(n)

    @pl.when(i >= MLP)
    def _():
        for n in (0, 1, 2, 3):
            update(n)


def adamw(g, total, weights, m, v):
    large = lambda i: jnp.minimum(i, MLP - 1)
    small = lambda i: lax.div(jnp.maximum(i - MLP, 0), 2)
    side = lambda i: lax.rem(jnp.maximum(i - MLP, 0), 2)

    def own(n):
        if n > 3:
            return pl.BlockSpec((1, D, D), (lambda i: (0, large(i), 0)) if n == 6 else (lambda i: (0, 0, large(i))))
        return pl.BlockSpec((1, HALF, D), (lambda i: (0, 2 * small(i) + side(i), 0)) if n == 3 else (lambda i: (0, side(i), small(i))))

    def part(n):
        if n > 3:
            return pl.BlockSpec((1, D, D), lambda i: (6 * lax.div(large(i), 2) + lax.rem(large(i), 2) + 2 * (n - 4), 0, 0))
        return pl.BlockSpec((1, HALF, D), lambda i: (3 * MLP + GROUPS * small(i) + n, side(i), 0))

    owns = [own(n) for n in range(7)]
    shapes = [jax.ShapeDtypeStruct(w.shape, BF16) for w in weights] + [jax.ShapeDtypeStruct(w.shape, F32) for w in weights] * 2
    return pl.pallas_call(
        functools.partial(_adamw_kernel, float(sum(w.size for w in weights))),
        grid=(MLP + 2 * GROUPS,),
        in_specs=[_whole(PIECE, HEAD)] + [part(n) for n in range(7)] + owns * 3,
        out_specs=owns * 3,
        out_shape=shapes,
        compiler_params=_params(),
        cost_estimate=_cost(2.5e8, 3.7e8, 1.7e7),
    )(total, *([g] * 7), *weights, *m, *v)


def solution(mesh):
    def step(x, dy, *arrays):
        weights, m, v = (arrays[i : i + 7] for i in (0, 7, 14))
        wq, wk, wv, wo, w_gate, w_up, w_down = weights
        x, dy = x[0], dy[0]
        cos, sin = tables(x.shape[0])
        q, k, value, at = qkv(x, wq, wk, wv, cos, sin)
        ot, lse, h, b, bt, dyt = attend(q, k, value, x, dy, wo)
        g, total = backward(b, bt, dy, dyt, w_gate, w_up, w_down, h, q, k, value, ot, lse, wo, at, cos, sin)
        return tuple(adamw(g, total, weights, m, v))

    states, all_of = P(("rep", "dp"), None, None), P(None, None, None)
    return jax.shard_map(
        step,
        mesh=mesh,
        in_specs=(states, states) + (all_of,) * 21,
        out_specs=(P("rep", None, None),) * 21,
        check_vma=False,
    )
```

```python
import functools

import jax
import jax.numpy as jnp
from jax import lax
from jax.experimental import pallas as pl
from jax.experimental.pallas import tpu as pltpu
from jax.sharding import PartitionSpec as P

F32, BF16 = jnp.float32, jnp.bfloat16
HIDDEN = -1e30
LOG2E = 1.4426950408889634
D, HALF, HEAD, QUARTER, EIGHTH, PIECE = 512, 256, 128, 64, 32, 16
THETA = 10000
VMEM = 63 * 2**20
ANY = "arbitrary"
MESH = pl.DeviceIdType.MESH
SCALE = HEAD**-0.5
E2 = SCALE * LOG2E


def _dot(a, b, ca=1, cb=0):
    return lax.dot_general(a, b, (((ca,), (cb,)), ((), ())), preferred_element_type=F32)


def _params(**more):
    return pltpu.CompilerParams(dimension_semantics=(ANY,), vmem_limit_bytes=VMEM, **more)


def _cost(flops, nbytes, exps=0):
    return pl.CostEstimate(flops=int(flops), bytes_accessed=int(nbytes), transcendentals=int(exps))


def _whole(*shape):
    return pl.BlockSpec(shape, lambda i: (0,) * len(shape), pipeline_mode=pl.Buffered(1))


def _col(i):
    return slice(i * HEAD, i * HEAD + HEAD)


def _norm_scale(wide):
    return lax.rsqrt(jnp.mean(wide * wide, -1, keepdims=True) + 1e-6)


def tables(tokens):
    half = HEAD // 2
    place = jnp.arange(HEAD)
    pace = THETA ** (-(place % half).astype(F32) / half)
    low = jnp.arange(EIGHTH, dtype=F32)[:, None] * pace
    high = (jnp.arange(tokens // EIGHTH, dtype=F32) * EIGHTH)[:, None] * pace
    sign = jnp.where(place < half, -1.0, 1.0)
    c, s, d, r = jnp.cos(high)[:, None], jnp.sin(high)[:, None], jnp.cos(low)[None], jnp.sin(low)[None]
    return (c * d - s * r).reshape(tokens, HEAD), ((s * d + c * r) * sign).reshape(tokens, HEAD)


BQ = HALF


def _front_kernel(x_ref, dy_ref, wq_ref, wk_ref, wv_ref, wo_ref, cos_ref, sin_ref, q_ref, k_ref, v_ref, at_ref, ot_ref, lse_ref, h_ref, b_ref, bt_ref,
                  dyt_ref, a_s, o_s, h_s, values_s):
    t = x_ref.shape[0]
    heads = range(D // HEAD)
    strips = [slice(r, r + BQ) for r in range(0, t, BQ)]

    @pl.when(pl.program_id(0) == 0)
    def _():
        for here in strips:
            wide = x_ref[here].astype(F32)
            a_s[here] = (wide * _norm_scale(wide)).astype(BF16)
        at_ref[...] = a_s[...].T
        dyt_ref[...] = dy_ref[...].T
        h_s[...] = jnp.zeros_like(h_s)
        for i in heads:
            values_s[i, HEAD:] = jnp.ones((PIECE, t), BF16)

    for here in strips:
        for w, out in ((wq_ref, q_ref), (wk_ref, k_ref)):
            whole = _dot(a_s[here], w[0]).astype(BF16).astype(F32)
            for i in heads:
                one = whole[:, _col(i)]
                out[here, _col(i)] = (one * cos_ref[here] + pltpu.roll(one, HEAD // 2, 1) * sin_ref[here]).astype(BF16)
        v_ref[here] = _dot(a_s[here], wv_ref[0]).astype(BF16)
    for i in heads:
        values_s[i, :HEAD] = v_ref[:, _col(i)].T

    hidden = lax.broadcasted_iota(jnp.int32, (BQ, BQ), 0) > lax.broadcasted_iota(jnp.int32, (BQ, BQ), 1)
    for n, here in enumerate(strips):
        scores = [[_dot(k_ref[keys, _col(i)], q_ref[here, _col(i)], 1, 1) for keys in strips[: n + 1]] for i in heads]
        weights, tops = [], []
        for s in scores:
            s[n] = jnp.where(hidden, HIDDEN, s[n])
            top = functools.reduce(jnp.maximum, [one.max(axis=0, keepdims=True) for one in s]) * E2
            weights.append(jnp.concatenate([jnp.exp2(one * E2 - top).astype(BF16) for one in s], axis=0))
            tops.append(top)
        for i in heads:
            mix = _dot(values_s[i, :, : here.stop], weights[i])
            total = mix[HEAD : HEAD + 1]
            out = (mix[:HEAD] * (1 / total)).astype(BF16)
            ot_ref[_col(i), here] = out
            o_s[here, _col(i)] = out.T
            lse_ref[i : i + 1, here] = tops[i] + jnp.log2(total)
    for here in strips:
        h_s[here] += _dot(o_s[here], wo_ref[0])

    @pl.when(pl.program_id(0) == pl.num_programs(0) - 1)
    def _():
        for here in strips:
            h = (x_ref[here].astype(F32) + h_s[here].astype(BF16).astype(F32)).astype(BF16)
            h_ref[here] = h
            wide = h.astype(F32)
            b = (wide * _norm_scale(wide)).astype(BF16)
            b_ref[here] = b
            bt_ref[:, here] = b.T


def front(x, dy, wq, wk, wv, wo, cos, sin):
    t, width = x.shape[0], wq.shape[2]
    n = width // D
    cols = pl.BlockSpec((t, D), lambda i: (0, i))
    w = pl.BlockSpec((1, D, D), lambda i: (0, 0, i))
    last = lambda *shape: pl.BlockSpec(shape, lambda i: (0, 0))
    shape = jax.ShapeDtypeStruct
    vm = pltpu.VMEM
    return pl.pallas_call(
        _front_kernel, grid=(n,), in_specs=[_whole(t, D), _whole(t, D), w, w, w, pl.BlockSpec((1, D, D), lambda i: (0, i, 0)), _whole(t, HEAD), _whole(t, HEAD)],
        out_specs=[cols, cols, cols, last(D, t), pl.BlockSpec((D, t), lambda i: (i, 0)), pl.BlockSpec((None, D // HEAD, t), lambda i: (i, 0, 0)),
                   last(t, D), last(t, D), last(D, t), last(D, t)],
        out_shape=[shape((t, width), BF16)] * 3 + [shape((D, t), BF16), shape((width, t), BF16), shape((n, D // HEAD, t), F32), shape((t, D), BF16),
                                                   shape((t, D), BF16), shape((D, t), BF16), shape((D, t), BF16)],
        scratch_shapes=[vm((t, D), BF16), vm((t, D), BF16), vm((t, D), F32), vm((D // HEAD, HEAD + PIECE, t), BF16)],
        compiler_params=_params(), cost_estimate=_cost(1.8e10, 4e7, 1e7),
    )(x, dy, wq, wk, wv, wo, cos, sin)


STRIDE = (32, 8, 2)
MLP, GROUPS, SUBS = 16, 4, 3
STEPS = MLP + GROUPS * SUBS
CHUNKS = 32
STAGES = 13
SMALL = MLP + 2 * SUBS
NEXT = SMALL + SUBS + 1
LAST = SMALL + 2 * SUBS
SLOTS = 9


def _reducer(grad, rd, s1, r1, s2, r2, p1, s3, r3, s4, r4, p2, s5, r5, fin, ebuf, acc, dsem, ssem, rsem, esem, out_ref, sum_ref):
    me = lax.axis_index("dp")
    core = lax.rem(me, 2)
    pos = [lax.rem(lax.div(me, s), 4) for s in STRIDE]
    partner = me + 1 - 2 * core

    def at(q, o):
        return jnp.where(q < 4 - o, q + o, q + o - 4)

    def peer(d, o):
        return me + jnp.where(pos[d] < 4 - o, o * STRIDE[d], (o - 4) * STRIDE[d])

    def begin():
        barrier = pltpu.get_barrier_semaphore()
        for dev in [partner] + [peer(d, o) for d in range(3) for o in (1, 2, 3)]:
            pl.semaphore_signal(barrier, inc=1, device_id={"dp": dev}, device_id_type=MESH)
        pl.semaphore_wait(barrier, 10)
        acc[...] = jnp.zeros_like(acc)

    rows = lambda start, n: pl.ds(pl.multiple_of(start, PIECE), n)
    lanes = lambda start, n: pl.ds(pl.multiple_of(start, HEAD), n)
    base = core * HALF

    def send(src, dst, kind, s, dev):
        return pltpu.make_async_remote_copy(src_ref=src, dst_ref=dst, send_sem=ssem.at[kind, s], recv_sem=rsem.at[kind, s],
                                            device_id={"dp": dev}, device_id_type=MESH)

    def stream(j):
        d1, d2, d3 = j, (j + 1) % 3, (j + 2) % 3
        q1, q2, q3 = pos[d1], pos[d2], pos[d3]
        row1 = base + q1 * QUARTER
        row2 = row1 + q2 * PIECE

        def copies(k, c, s):
            right1, left1, right2, left2 = peer(d1, 1), peer(d1, 3), peer(d2, 1), peer(d2, 3)
            home = lambda row, n, lane=pl.ds(0, D): out_ref.at[pl.ds(2 * c, 2), rows(row, n), lane]
            if k == 0:
                return [send(grad.at[s, :, rows(HALF - base, HALF), :], rd.at[s], 0, s, partner)]
            if k in (1, 2, 3, 4):
                src, dst = ((s1, r1), (s2, r2), (s3, r3), (s4, r4))[k - 1]
                right, left = (right1, left1) if k < 3 else (right2, left2)
                return [send(src.at[s, 0], dst.at[s, 0], 2 * k - 1, s, right), send(src.at[s, 1], dst.at[s, 1], 2 * k, s, left)]
            if k == 5:
                return [send(s5.at[s, o - 1], r5.at[s, o - 1], 8 + o, s, peer(d3, o)) for o in (1, 2, 3)]
            if k == 6:
                mine = home(row2, PIECE, lanes(q3 * HEAD, HEAD))
                return [pltpu.make_async_copy(fin.at[s], mine, dsem.at[s])] + [send(fin.at[s], mine, 11 + o, s, peer(d3, o)) for o in (1, 2, 3)]
            if k == 7:
                mine = home(row2, PIECE)
                return [send(mine, mine, 15, s, right2), send(mine, mine, 16, s, left2)]
            if k == 8:
                a = home(row1 + at(q2, 3) * PIECE, PIECE, pl.ds(0, HALF))
                z = home(row1 + at(q2, 1) * PIECE, PIECE, pl.ds(HALF, HALF))
                return [send(a, a, 17, s, right2), send(z, z, 18, s, left2)]
            if k == 9:
                mine = home(row1, QUARTER)
                return [send(mine, mine, 19, s, right1), send(mine, mine, 20, s, left1)]
            if k == 10:
                a = home(base + at(q1, 3) * QUARTER, EIGHTH)
                z = home(base + at(q1, 1) * QUARTER + EIGHTH, EIGHTH)
                return [send(a, a, 21, s, right1), send(z, z, 22, s, left1)]
            if k == 11:
                mine = home(base, HALF)
                return [send(mine, mine, 23, s, partner)]
            return []

        def work(k, s):
            def both(start, n):
                return grad[s, :, rows(base + start, n), :].astype(F32) + rd[s, :, rows(start, n), :].astype(F32)

            if k == 1:
                far = at(q1, 2) * QUARTER
                s1[s, 0] = both(far, EIGHTH).astype(BF16)
                s1[s, 1] = both(far + EIGHTH, EIGHTH).astype(BF16)
                p1[s] = both(q1 * QUARTER, QUARTER)
            if k == 2:
                a, z = at(q1, 1) * QUARTER, at(q1, 3) * QUARTER
                s2[s, 0, :, :EIGHTH] = (both(a, EIGHTH) + r1[s, 0].astype(F32)).astype(BF16)
                s2[s, 0, :, EIGHTH:] = both(a + EIGHTH, EIGHTH).astype(BF16)
                s2[s, 1, :, :EIGHTH] = both(z, EIGHTH).astype(BF16)
                s2[s, 1, :, EIGHTH:] = (both(z + EIGHTH, EIGHTH) + r1[s, 1].astype(F32)).astype(BF16)
            if k == 3:
                p1[s] += r2[s, 0].astype(F32) + r2[s, 1].astype(F32)
                far = p1[s, :, rows(at(q2, 2) * PIECE, PIECE), :].astype(BF16)
                s3[s, 0] = far[:, :, :HALF]
                s3[s, 1] = far[:, :, HALF:]
            if k == 4:
                a, z = p1[s, :, rows(at(q2, 1) * PIECE, PIECE), :], p1[s, :, rows(at(q2, 3) * PIECE, PIECE), :]
                s4[s, 0, :, :, :HALF] = (a[:, :, :HALF] + r3[s, 0].astype(F32)).astype(BF16)
                s4[s, 0, :, :, HALF:] = a[:, :, HALF:].astype(BF16)
                s4[s, 1, :, :, :HALF] = z[:, :, :HALF].astype(BF16)
                s4[s, 1, :, :, HALF:] = (z[:, :, HALF:] + r3[s, 1].astype(F32)).astype(BF16)
            if k == 5:
                p2[s] = p1[s, :, rows(q2 * PIECE, PIECE), :] + r4[s, 0].astype(F32) + r4[s, 1].astype(F32)
                for o in (1, 2, 3):
                    s5[s, o - 1] = p2[s, :, :, lanes(at(q3, o) * HEAD, HEAD)].astype(BF16)
            if k == 6:
                total = p2[s, :, :, lanes(q3 * HEAD, HEAD)]
                for o in (1, 2, 3):
                    total += r5[s, o - 1].astype(F32)
                total = total.astype(BF16)
                fin[s] = total
                square = total.astype(F32) * total.astype(F32)
                acc[...] += square[0] + square[1]

        return copies, work

    streams = [stream(j) for j in range(3)]

    def stage(t, k):
        u = t - k
        of_large = (u >= 2) & (u <= MLP)

        @pl.when(of_large | (u == SMALL) | (u == NEXT) | (u == LAST))
        def _():
            triple = jnp.where(u <= MLP, lax.div(u, 2) - 1, MLP // 2 + jnp.where(u < LAST, jnp.where(u > SMALL, 1, 0), 2))
            c, s = 3 * triple, 3 * lax.rem(triple, 3)

            def run(some):
                if k > 0:
                    for j in some:
                        for copy in streams[j][0](k - 1, c + j, s + j):
                            copy.wait()
                for j in some:
                    streams[j][1](k, s + j)
                for j in some:
                    for copy in streams[j][0](k, c + j, s + j):
                        copy.start()

            run((0, 1))
            pl.when(u < LAST)(lambda: run((2,)))

    def hops(k):
        if k == 3:
            return [(0, core, partner)]
        return [(o - 1, pos[k], peer(k, o)) for o in (1, 2, 3)]

    def moves(k):
        return [pltpu.make_async_remote_copy(src_ref=ebuf.at[k, place], dst_ref=ebuf.at[k, place], send_sem=esem.at[0, k, n],
                                             recv_sem=esem.at[1, k, n], device_id={"dp": dev}, device_id_type=MESH)
                for n, place, dev in hops(k)]

    def exchange(k):
        if k > 0:
            for copy in moves(k - 1):
                copy.wait()
            total = ebuf[k - 1, 0] + ebuf[k - 1, 1]
            if k < 4:
                total = total + ebuf[k - 1, 2] + ebuf[k - 1, 3]
        else:
            total = acc[...]
        if k == 4:
            sum_ref[...] = total
        else:
            ebuf[k, hops(k)[0][1]] = total
            for copy in moves(k):
                copy.start()

    def tick(t):
        for odd in (0, 1):

            @pl.when(lax.rem(t, 2) == odd)
            def _():
                for k in range(STAGES - 2 + (1 - odd), -1, -2):
                    stage(t, k)

    def finish():
        def late(t, _):
            tick(t)
            for k in range(5):
                pl.when(t == LAST + 7 + k)(functools.partial(exchange, k))

        lax.fori_loop(STEPS, LAST + STAGES, late, None)

    return begin, tick, finish


def _mlp_step(i, b_ref, bt_ref, dy_ref, dyt_ref, wg_ref, wu_ref, wd_ref, h_ref, grad, db_s, dh_s, hid_s, dg_s, du_s):
    t = b_ref.shape[0]
    parts = [slice(r, r + D) for r in range(0, t, D)]

    @pl.when(i == 0)
    def _():
        db_s[...] = jnp.zeros_like(db_s)

    wg, wu, wd = wg_ref[0], wu_ref[0], wd_ref[0]
    for here in parts:
        gate, up = _dot(b_ref[here], wg), _dot(b_ref[here], wu)
        dh = _dot(dy_ref[here], wd, 1, 1).astype(BF16).astype(F32)
        sig = 0.5 * jnp.tanh(0.5 * gate) + 0.5
        act = gate * sig
        hid_s[here] = (act * up).astype(BF16)
        du_s[here] = (dh * act).astype(BF16)
        dg_s[here] = (dh * up * (sig + act * (1 - sig))).astype(BF16)
    for here in parts:
        db_s[here] += _dot(dg_s[here], wg, 1, 1) + _dot(du_s[here], wu, 1, 1)
    first, n = 3 * lax.div(i, 2), lax.rem(i, 2)
    grad[lax.rem(first, SLOTS), n] = _dot(bt_ref[...], dg_s[...]).astype(BF16)
    grad[lax.rem(first + 1, SLOTS), n] = _dot(bt_ref[...], du_s[...]).astype(BF16)
    grad[lax.rem(first + 2, SLOTS), n] = _dot(dyt_ref[...], hid_s[...]).astype(BF16)

    @pl.when(i == MLP - 1)
    def _():
        for here in parts:
            db = db_s[here].astype(BF16).astype(F32)
            wide = h_ref[here].astype(F32)
            scale = _norm_scale(wide)
            inner = jnp.mean(db * wide, -1, keepdims=True)
            dh_s[here] = (dy_ref[here].astype(F32) + (db * scale - wide * (scale * scale * scale * inner))).astype(BF16)


def _attend_step(g, sub, q_ref, k_ref, v_ref, ot_ref, lse_ref, wo_ref, at_ref, cos_ref, sin_ref, grad, dh_s, dot_s, delta_s, dq_s, dk_s, dv_s):
    t = q_ref.shape[0]
    heads = range(q_ref.shape[1] // HEAD)
    half = t // 2
    hidden = lax.broadcasted_iota(jnp.int32, (BQ, BQ), 0) > lax.broadcasted_iota(jnp.int32, (BQ, BQ), 1)
    first = lax.rem(CHUNKS - 2 * GROUPS + 2 * g, SLOTS)
    second = lax.rem(first + 1, SLOTS)

    def block(a, end, j):
        queries, keys = slice(a, end), slice(j, j + BQ)
        scores = [_dot(k_ref[keys, _col(i)], q_ref[queries, _col(i)], 1, 1) for i in heads]
        dps = [_dot(v_ref[keys, _col(i)], dot_s[_col(i), queries]) for i in heads]
        for i in heads:
            p = jnp.exp2(scores[i] * E2 - lse_ref[i : i + 1, queries])
            if a == j:
                cut = jnp.where(hidden, 0.0, p[:, :BQ])
                p = cut if end - a == BQ else jnp.concatenate([cut, p[:, BQ:]], axis=1)
            ds = (p * (dps[i] - delta_s[i : i + 1, queries])).astype(BF16)
            dv_s[keys, _col(i)] += _dot(p.astype(BF16), dot_s[_col(i), queries], 1, 1)
            dk_s[keys, _col(i)] += _dot(ds, q_ref[queries, _col(i)])
            dq_s[_col(i), queries] += _dot(k_ref[keys, _col(i)].T, ds)

    def turned_back(one):
        one = (one * SCALE).astype(BF16).astype(F32)
        return (one * cos_ref[...] - pltpu.roll(one, HEAD // 2, 1) * sin_ref[...]).astype(BF16)

    @pl.when(sub == 0)
    def _():
        dot_s[...] = _dot(wo_ref[0], dh_s[...], 1, 1).astype(BF16)
        grad[second, 1] = _dot(ot_ref[...], dh_s[...]).astype(BF16)
        for i in heads:
            delta_s[i : i + 1, :] = jnp.sum(dot_s[_col(i), :].astype(F32) * ot_ref[_col(i), :].astype(F32), axis=0, keepdims=True)
        for total in (dq_s, dk_s, dv_s):
            total[...] = jnp.zeros_like(total)
        for j in range(0, half, BQ):
            block(j, half, j)

    @pl.when(sub == 1)
    def _():
        for j in range(0, half, BQ):
            block(half, t, j)

    @pl.when(sub == 2)
    def _():
        for j in range(half, t, BQ):
            block(j, t, j)
        grad[second, 0] = _dot(at_ref[...], dv_s[...].astype(BF16)).astype(BF16)
        dk = jnp.concatenate([turned_back(dk_s[:, _col(i)]) for i in heads], axis=1)
        grad[first, 1] = _dot(at_ref[...], dk).astype(BF16)
        dq = jnp.concatenate([turned_back(dq_s[_col(i), :].T) for i in heads], axis=1)
        grad[first, 0] = _dot(at_ref[...], dq).astype(BF16)


def _backward_kernel(b_ref, bt_ref, dy_ref, dyt_ref, wg_ref, wu_ref, wd_ref, h_ref, q_ref, k_ref, v_ref, ot_ref, lse_ref, wo_ref, at_ref, cos_ref,
                     sin_ref, out_ref, sum_ref, dh_s, hid_s, dg_s, du_s, dot_s, delta_s, dq_s, dk_s, dv_s, grad, *rest):
    p = pl.program_id(0)
    begin, tick, finish = _reducer(grad, *rest, out_ref, sum_ref)
    pl.when(p == 0)(begin)
    tick(p)

    @pl.when(p < MLP)
    def _():
        _mlp_step(p, b_ref, bt_ref, dy_ref, dyt_ref, wg_ref, wu_ref, wd_ref, h_ref, grad, dk_s, dh_s, hid_s, dg_s, du_s)

    @pl.when(p >= MLP)
    def _():
        _attend_step(lax.div(p - MLP, SUBS), lax.rem(p - MLP, SUBS), q_ref, k_ref, v_ref, ot_ref, lse_ref, wo_ref, at_ref, cos_ref, sin_ref, grad, dh_s,
                     dot_s, delta_s, dq_s, dk_s, dv_s)

    pl.when(p == STEPS - 1)(finish)


def backward(b, bt, dy, dyt, wg, wu, wd, h, q, k, v, ot, lse, wo, at, cos, sin):
    t = b.shape[0]
    large = lambda p: jnp.minimum(p, MLP - 1)
    group = lambda p: lax.div(jnp.clip(p - MLP, 0, GROUPS * SUBS - 1), SUBS)
    cols = pl.BlockSpec((1, D, D), lambda p: (0, 0, large(p)))
    heads = pl.BlockSpec((t, D), lambda p: (0, group(p)))
    vm, sem = pltpu.VMEM, pltpu.SemaphoreType.DMA
    two = lambda *shape: vm((SLOTS, 2, 2) + shape, BF16)
    three = vm((SLOTS, 3, 2, PIECE, HEAD), BF16)
    return pl.pallas_call(
        _backward_kernel, grid=(STEPS,),
        in_specs=[_whole(t, D), _whole(D, t), _whole(t, D), _whole(D, t), cols, cols, pl.BlockSpec((1, D, D), lambda p: (0, large(p), 0)), _whole(t, D),
                  heads, heads, heads, pl.BlockSpec((D, t), lambda p: (group(p), 0)), pl.BlockSpec((None,) + lse.shape[1:], lambda p: (group(p), 0, 0)),
                  pl.BlockSpec((1, D, D), lambda p: (0, group(p), 0)), _whole(D, t), _whole(t, HEAD), _whole(t, HEAD)],
        out_specs=[pl.BlockSpec(memory_space=pl.ANY), pl.BlockSpec((PIECE, HEAD), lambda p: (0, 0))],
        out_shape=[jax.ShapeDtypeStruct((2 * CHUNKS, D, D), BF16), jax.ShapeDtypeStruct((PIECE, HEAD), F32)],
        scratch_shapes=[vm((t, D), BF16), vm((t, D), BF16), vm((t, D), BF16), vm((t, D), BF16), vm((D, t), BF16), vm((4, t), F32), vm((D, t), F32),
                        vm((t, D), F32), vm((t, D), F32), vm((SLOTS, 2, D, D), BF16), vm((SLOTS, 2, HALF, D), BF16), two(EIGHTH, D), two(EIGHTH, D),
                        two(QUARTER, D), two(QUARTER, D), vm((SLOTS, 2, QUARTER, D), F32), two(PIECE, HALF), two(PIECE, HALF), two(PIECE, D),
                        two(PIECE, D), vm((SLOTS, 2, PIECE, D), F32), three, three, vm((SLOTS, 2, PIECE, HEAD), BF16), vm((4, 4, PIECE, HEAD), F32),
                        vm((PIECE, HEAD), F32), sem((SLOTS,)), sem((24, SLOTS)), sem((24, SLOTS)), sem((2, 4, 3))],
        compiler_params=_params(collective_id=0, has_side_effects=True), cost_estimate=_cost(1.1e11, 1e8, 2e7),
    )(b, bt, dy, dyt, wg, wu, wd, h, q, k, v, ot, lse, wo, at, cos, sin)


def _adamw_kernel(count, sum_ref, *refs):
    g, w, m, v, new_w, new_m, new_v = (refs[7 * i : 7 * i + 7] for i in range(7))
    i = pl.program_id(0)
    factor = jnp.minimum(1.0, 0.5 * lax.rsqrt(jnp.sum(sum_ref[...], keepdims=True) / count + 1e-30))

    def update(n):
        def some(r, _):
            here = pl.ds(pl.multiple_of(r * HEAD, HEAD), HEAD)
            gradient = (g[n][0, :, here].T if n == 6 else g[n][0, here, :]).astype(F32) * factor
            mean = 0.9 * m[n][0, here, :] + 0.1 * gradient
            square = 0.95 * v[n][0, here, :] + 0.05 * gradient * gradient
            weight = w[n][0, here, :].astype(F32)
            step = mean * lax.rsqrt(square + 1e-8) + 0.1 * weight
            new_w[n][0, here, :] = (weight - 0.02 * step).astype(BF16)
            new_m[n][0, here, :] = mean
            new_v[n][0, here, :] = square

        lax.fori_loop(0, m[n].shape[1] // HEAD, some, None)

    @pl.when(i < MLP)
    def _():
        for n in (4, 5, 6):
            update(n)

    @pl.when(i >= MLP)
    def _():
        for n in (0, 1, 2, 3):
            update(n)


def adamw(g, total, weights, m, v):
    large = lambda i: jnp.minimum(i, MLP - 1)
    small = lambda i: lax.div(jnp.maximum(i - MLP, 0), 2)
    side = lambda i: lax.rem(jnp.maximum(i - MLP, 0), 2)

    def own(n):
        if n > 3:
            return pl.BlockSpec((1, D, D), (lambda i: (0, large(i), 0)) if n == 6 else (lambda i: (0, 0, large(i))))
        return pl.BlockSpec((1, HALF, D), (lambda i: (0, 2 * small(i) + side(i), 0)) if n == 3 else (lambda i: (0, side(i), small(i))))

    def part(n):
        if n > 3:
            return pl.BlockSpec((1, D, D), lambda i: (6 * lax.div(large(i), 2) + lax.rem(large(i), 2) + 2 * (n - 4), 0, 0))
        return pl.BlockSpec((1, HALF, D), lambda i: (3 * MLP + GROUPS * small(i) + n, side(i), 0))

    owns = [own(n) for n in range(7)]
    shapes = [jax.ShapeDtypeStruct(w.shape, BF16) for w in weights] + [jax.ShapeDtypeStruct(w.shape, F32) for w in weights] * 2
    return pl.pallas_call(
        functools.partial(_adamw_kernel, float(sum(w.size for w in weights))),
        grid=(MLP + 2 * GROUPS,),
        in_specs=[_whole(PIECE, HEAD)] + [part(n) for n in range(7)] + owns * 3,
        out_specs=owns * 3,
        out_shape=shapes,
        compiler_params=_params(),
        cost_estimate=_cost(2.5e8, 3.7e8, 1.7e7),
    )(total, *([g] * 7), *weights, *m, *v)


def solution(mesh):
    def step(x, dy, *arrays):
        weights, m, v = (arrays[i : i + 7] for i in (0, 7, 14))
        wq, wk, wv, wo, w_gate, w_up, w_down = weights
        x, dy = x[0], dy[0]
        cos, sin = tables(x.shape[0])
        q, k, value, at, ot, lse, h, b, bt, dyt = front(x, dy, wq, wk, wv, wo, cos, sin)
        g, total = backward(b, bt, dy, dyt, w_gate, w_up, w_down, h, q, k, value, ot, lse, wo, at, cos, sin)
        return tuple(adamw(g, total, weights, m, v))

    states, all_of = P(("rep", "dp"), None, None), P(None, None, None)
    return jax.shard_map(
        step,
        mesh=mesh,
        in_specs=(states, states) + (all_of,) * 21,
        out_specs=(P("rep", None, None),) * 21,
        check_vma=False,
    )
```

```python
import functools

import jax
import jax.numpy as jnp
from jax import lax
from jax.experimental import pallas as pl
from jax.experimental.pallas import tpu as pltpu
from jax.sharding import PartitionSpec as P

F32, BF16 = jnp.float32, jnp.bfloat16
HIDDEN = -1e30
LOG2E = 1.4426950408889634
D, HALF, HEAD, QUARTER, EIGHTH, PIECE = 512, 256, 128, 64, 32, 16
THETA = 10000
VMEM = 63 * 2**20
ANY = "arbitrary"
MESH = pl.DeviceIdType.MESH
SCALE = HEAD**-0.5
E2 = SCALE * LOG2E


def _dot(a, b, ca=1, cb=0):
    return lax.dot_general(a, b, (((ca,), (cb,)), ((), ())), preferred_element_type=F32)


def _params(**more):
    return pltpu.CompilerParams(dimension_semantics=(ANY,), vmem_limit_bytes=VMEM, **more)


def _cost(flops, nbytes, exps=0):
    return pl.CostEstimate(flops=int(flops), bytes_accessed=int(nbytes), transcendentals=int(exps))


def _whole(*shape):
    return pl.BlockSpec(shape, lambda i: (0,) * len(shape), pipeline_mode=pl.Buffered(1))


def _col(i):
    return slice(i * HEAD, i * HEAD + HEAD)


def _norm_scale(wide):
    return lax.rsqrt(jnp.mean(wide * wide, -1, keepdims=True) + 1e-6)


def tables(tokens):
    half = HEAD // 2
    place = jnp.arange(HEAD)
    pace = THETA ** (-(place % half).astype(F32) / half)
    low = jnp.arange(EIGHTH, dtype=F32)[:, None] * pace
    high = (jnp.arange(tokens // EIGHTH, dtype=F32) * EIGHTH)[:, None] * pace
    sign = jnp.where(place < half, -1.0, 1.0)
    c, s, d, r = jnp.cos(high)[:, None], jnp.sin(high)[:, None], jnp.cos(low)[None], jnp.sin(low)[None]
    return (c * d - s * r).reshape(tokens, HEAD), ((s * d + c * r) * sign).reshape(tokens, HEAD)


BQ = HALF


def _front_kernel(x_ref, dy_ref, wq_ref, wk_ref, wv_ref, wo_ref, cos_ref, sin_ref, q_ref, k_ref, v_ref, at_ref, ot_ref, lse_ref, h_ref, b_ref, bt_ref,
                  dyt_ref, a_s, o_s, h_s, values_s):
    t = x_ref.shape[0]
    heads = range(D // HEAD)
    strips = [slice(r, r + BQ) for r in range(0, t, BQ)]

    @pl.when(pl.program_id(0) == 0)
    def _():
        for here in strips:
            wide = x_ref[here].astype(F32)
            a_s[here] = (wide * _norm_scale(wide)).astype(BF16)
        at_ref[...] = a_s[...].T
        dyt_ref[...] = dy_ref[...].T
        h_s[...] = jnp.zeros_like(h_s)
        for i in heads:
            values_s[i, HEAD:] = jnp.ones((PIECE, t), BF16)

    for here in strips:
        for w, out in ((wq_ref, q_ref), (wk_ref, k_ref)):
            whole = _dot(a_s[here], w[0]).astype(BF16).astype(F32)
            for i in heads:
                one = whole[:, _col(i)]
                out[here, _col(i)] = (one * cos_ref[here] + pltpu.roll(one, HEAD // 2, 1) * sin_ref[here]).astype(BF16)
        v_ref[here] = _dot(a_s[here], wv_ref[0]).astype(BF16)
    for i in heads:
        values_s[i, :HEAD] = v_ref[:, _col(i)].T

    hidden = lax.broadcasted_iota(jnp.int32, (BQ, BQ), 0) > lax.broadcasted_iota(jnp.int32, (BQ, BQ), 1)
    for n, here in enumerate(strips):
        scores = [[_dot(k_ref[keys, _col(i)], q_ref[here, _col(i)], 1, 1) for keys in strips[: n + 1]] for i in heads]
        weights, tops = [], []
        for s in scores:
            s[n] = jnp.where(hidden, HIDDEN, s[n])
            top = functools.reduce(jnp.maximum, [one.max(axis=0, keepdims=True) for one in s]) * E2
            weights.append(jnp.concatenate([jnp.exp2(one * E2 - top).astype(BF16) for one in s], axis=0))
            tops.append(top)
        for i in heads:
            mix = _dot(values_s[i, :, : here.stop], weights[i])
            total = mix[HEAD : HEAD + 1]
            out = (mix[:HEAD] * (1 / total)).astype(BF16)
            ot_ref[_col(i), here] = out
            o_s[here, _col(i)] = out.T
            lse_ref[i : i + 1, here] = tops[i] + jnp.log2(total)
    for here in strips:
        h_s[here] += _dot(o_s[here], wo_ref[0])

    @pl.when(pl.program_id(0) == pl.num_programs(0) - 1)
    def _():
        for here in strips:
            h = (x_ref[here].astype(F32) + h_s[here].astype(BF16).astype(F32)).astype(BF16)
            h_ref[here] = h
            wide = h.astype(F32)
            b = (wide * _norm_scale(wide)).astype(BF16)
            b_ref[here] = b
            bt_ref[:, here] = b.T


def front(x, dy, wq, wk, wv, wo, cos, sin):
    t, width = x.shape[0], wq.shape[2]
    n = width // D
    cols = pl.BlockSpec((t, D), lambda i: (0, i))
    w = pl.BlockSpec((1, D, D), lambda i: (0, 0, i))
    last = lambda *shape: pl.BlockSpec(shape, lambda i: (0, 0))
    shape = jax.ShapeDtypeStruct
    vm = pltpu.VMEM
    return pl.pallas_call(
        _front_kernel, grid=(n,), in_specs=[_whole(t, D), _whole(t, D), w, w, w, pl.BlockSpec((1, D, D), lambda i: (0, i, 0)), _whole(t, HEAD), _whole(t, HEAD)],
        out_specs=[cols, cols, cols, last(D, t), pl.BlockSpec((D, t), lambda i: (i, 0)), pl.BlockSpec((None, D // HEAD, t), lambda i: (i, 0, 0)),
                   last(t, D), last(t, D), last(D, t), last(D, t)],
        out_shape=[shape((t, width), BF16)] * 3 + [shape((D, t), BF16), shape((width, t), BF16), shape((n, D // HEAD, t), F32), shape((t, D), BF16),
                                                   shape((t, D), BF16), shape((D, t), BF16), shape((D, t), BF16)],
        scratch_shapes=[vm((t, D), BF16), vm((t, D), BF16), vm((t, D), F32), vm((D // HEAD, HEAD + PIECE, t), BF16)],
        compiler_params=_params(), cost_estimate=_cost(1.8e10, 4e7, 1e7),
    )(x, dy, wq, wk, wv, wo, cos, sin)


STRIDE = (32, 8, 2)
MLP, GROUPS, SUBS = 16, 4, 3
STEPS = MLP + GROUPS * SUBS
CHUNKS = 32
STAGES = 13
SMALL = MLP + 2 * SUBS
NEXT = SMALL + SUBS + 1
SLOTS = 9


def _reducer(grad, rd, s1, r1, s2, r2, p1, s3, r3, s4, r4, p2, s5, r5, fin, ebuf, acc, dsem, ssem, rsem, esem, out_ref, sum_ref):
    me = lax.axis_index("dp")
    core = lax.rem(me, 2)
    pos = [lax.rem(lax.div(me, s), 4) for s in STRIDE]
    partner = me + 1 - 2 * core

    def at(q, o):
        return jnp.where(q < 4 - o, q + o, q + o - 4)

    def peer(d, o):
        return me + jnp.where(pos[d] < 4 - o, o * STRIDE[d], (o - 4) * STRIDE[d])

    def begin():
        barrier = pltpu.get_barrier_semaphore()
        for dev in [partner] + [peer(d, o) for d in range(3) for o in (1, 2, 3)]:
            pl.semaphore_signal(barrier, inc=1, device_id={"dp": dev}, device_id_type=MESH)
        pl.semaphore_wait(barrier, 10)
        acc[...] = jnp.zeros_like(acc)

    rows = lambda start, n: pl.ds(pl.multiple_of(start, PIECE), n)
    lanes = lambda start, n: pl.ds(pl.multiple_of(start, HEAD), n)
    base = core * HALF

    def remote(src, dst, k, third, dev):
        return pltpu.make_async_remote_copy(src_ref=src, dst_ref=dst, send_sem=ssem.at[k, third], recv_sem=rsem.at[k, third],
                                            device_id={"dp": dev}, device_id_type=MESH)

    def wait(k, third, streams, late):
        same = (rd, r1, r2, r3, r4, r5, r5, r4, r3, r2, r1, rd)[k].at[pl.ds(3 * third, streams)]
        remote(same, same, k, third, partner).wait()
        if k == (11 if late else 6):
            same = (rd if late else fin).at[pl.ds(3 * third, streams)]
            pltpu.make_async_copy(same, same, dsem.at[third]).wait()

    def stream(j):
        d1, d2, d3 = j, (j + 1) % 3, (j + 2) % 3
        q1, q2, q3 = pos[d1], pos[d2], pos[d3]
        row1 = q1 * QUARTER
        row2 = row1 + q2 * PIECE

        def copies(k, c, third, late=False):
            s = 3 * third + j
            send = lambda src, dst, dev: remote(src, dst, k, third, dev)
            right1, left1, right2, left2 = peer(d1, 1), peer(d1, 3), peer(d2, 1), peer(d2, 3)

            def home(row, n, lane=pl.ds(0, D)):
                return rd.at[s, :, rows(row, n), lane] if late else out_ref.at[pl.ds(2 * c, 2), rows(base + row, n), lane]

            if k == 0:
                return [send(grad.at[s, :, rows(HALF - base, HALF), :], rd.at[s], partner)]
            if k in (1, 2, 3, 4):
                src, dst = ((s1, r1), (s2, r2), (s3, r3), (s4, r4))[k - 1]
                right, left = (right1, left1) if k < 3 else (right2, left2)
                return [send(src.at[s, 0], dst.at[s, 0], right), send(src.at[s, 1], dst.at[s, 1], left)]
            if k == 5:
                return [send(s5.at[s, o - 1], r5.at[s, o - 1], peer(d3, o)) for o in (1, 2, 3)]
            if k == 6:
                mine = home(row2, PIECE, lanes(q3 * HEAD, HEAD))
                own = [] if late else [pltpu.make_async_copy(fin.at[s], mine, dsem.at[third])]
                return own + [send(fin.at[s], mine, peer(d3, o)) for o in (1, 2, 3)]
            if k == 7:
                mine = home(row2, PIECE)
                return [send(mine, mine, right2), send(mine, mine, left2)]
            if k == 8:
                a = home(row1 + at(q2, 3) * PIECE, PIECE, pl.ds(0, HALF))
                z = home(row1 + at(q2, 1) * PIECE, PIECE, pl.ds(HALF, HALF))
                return [send(a, a, right2), send(z, z, left2)]
            if k == 9:
                mine = home(row1, QUARTER)
                return [send(mine, mine, right1), send(mine, mine, left1)]
            if k == 10:
                a = home(at(q1, 3) * QUARTER, EIGHTH)
                z = home(at(q1, 1) * QUARTER + EIGHTH, EIGHTH)
                return [send(a, a, right1), send(z, z, left1)]
            if k == 11:
                mine, goal = home(0, HALF), out_ref.at[pl.ds(2 * c, 2), rows(base, HALF), :]
                own = [pltpu.make_async_copy(mine, goal, dsem.at[third])] if late else []
                return own + [send(mine, goal, partner)]
            return []

        def work(k, s, late=False):
            def both(start, n):
                return grad[s, :, rows(base + start, n), :].astype(F32) + rd[s, :, rows(start, n), :].astype(F32)

            if k == 1:
                far = at(q1, 2) * QUARTER
                s1[s, 0] = both(far, EIGHTH).astype(BF16)
                s1[s, 1] = both(far + EIGHTH, EIGHTH).astype(BF16)
                p1[s] = both(q1 * QUARTER, QUARTER)
            if k == 2:
                a, z = at(q1, 1) * QUARTER, at(q1, 3) * QUARTER
                s2[s, 0, :, :EIGHTH] = (both(a, EIGHTH) + r1[s, 0].astype(F32)).astype(BF16)
                s2[s, 0, :, EIGHTH:] = both(a + EIGHTH, EIGHTH).astype(BF16)
                s2[s, 1, :, :EIGHTH] = both(z, EIGHTH).astype(BF16)
                s2[s, 1, :, EIGHTH:] = (both(z + EIGHTH, EIGHTH) + r1[s, 1].astype(F32)).astype(BF16)
            if k == 3:
                p1[s] += r2[s, 0].astype(F32) + r2[s, 1].astype(F32)
                far = p1[s, :, rows(at(q2, 2) * PIECE, PIECE), :].astype(BF16)
                s3[s, 0] = far[:, :, :HALF]
                s3[s, 1] = far[:, :, HALF:]
            if k == 4:
                a, z = p1[s, :, rows(at(q2, 1) * PIECE, PIECE), :], p1[s, :, rows(at(q2, 3) * PIECE, PIECE), :]
                s4[s, 0, :, :, :HALF] = (a[:, :, :HALF] + r3[s, 0].astype(F32)).astype(BF16)
                s4[s, 0, :, :, HALF:] = a[:, :, HALF:].astype(BF16)
                s4[s, 1, :, :, :HALF] = z[:, :, :HALF].astype(BF16)
                s4[s, 1, :, :, HALF:] = (z[:, :, HALF:] + r3[s, 1].astype(F32)).astype(BF16)
            if k == 5:
                p2[s] = p1[s, :, rows(q2 * PIECE, PIECE), :] + r4[s, 0].astype(F32) + r4[s, 1].astype(F32)
                for o in (1, 2, 3):
                    s5[s, o - 1] = p2[s, :, :, lanes(at(q3, o) * HEAD, HEAD)].astype(BF16)
            if k == 6:
                total = p2[s, :, :, lanes(q3 * HEAD, HEAD)]
                for o in (1, 2, 3):
                    total += r5[s, o - 1].astype(F32)
                total = total.astype(BF16)
                fin[s] = total
                if late:
                    rd[s, :, rows(row2, PIECE), lanes(q3 * HEAD, HEAD)] = total
                square = total.astype(F32) * total.astype(F32)
                acc[...] += square[0] + square[1]

        return copies, work

    streams = [stream(j) for j in range(3)]

    def run(k, triple, third, number=3, late=False):
        if k > 0:
            wait(k - 1, third, number, late)
        for j in range(number):
            streams[j][1](k, 3 * third + j, late)
        for j in range(number):
            for copy in streams[j][0](k, 3 * triple + j, third, late):
                copy.start()

    def stage(t, k):
        u = t - k
        now = (u >= 2) & (u <= MLP)
        if k + SMALL < STEPS:
            now = now | (u == SMALL)
        if k + NEXT < STEPS:
            now = now | (u == NEXT)

        @pl.when(now)
        def _():
            triple = jnp.where(u <= MLP, lax.div(u, 2) - 1, MLP // 2 + jnp.where(u > SMALL, 1, 0))
            run(k, triple, lax.rem(triple, 3))

    def hops(k):
        if k == 3:
            return [(0, core, partner)]
        return [(o - 1, pos[k], peer(k, o)) for o in (1, 2, 3)]

    def moves(k):
        return [pltpu.make_async_remote_copy(src_ref=ebuf.at[k, place], dst_ref=ebuf.at[k, place], send_sem=esem.at[0, k, n],
                                             recv_sem=esem.at[1, k, n], device_id={"dp": dev}, device_id_type=MESH)
                for n, place, dev in hops(k)]

    def exchange(k):
        if k > 0:
            for copy in moves(k - 1):
                copy.wait()
            total = ebuf[k - 1, 0] + ebuf[k - 1, 1]
            if k < 4:
                total = total + ebuf[k - 1, 2] + ebuf[k - 1, 3]
        else:
            total = acc[...]
        if k == 4:
            sum_ref[...] = total
        else:
            ebuf[k, hops(k)[0][1]] = total
            for copy in moves(k):
                copy.start()

    def tick(t):
        for odd in (0, 1):

            @pl.when(lax.rem(t, 2) == odd)
            def _():
                for k in range(STAGES - 2 + (1 - odd), -1, -2):
                    stage(t, k)

    def finish():
        final = MLP // 2 + 2
        firsts = {final: STEPS, final - 1: NEXT, final - 2: SMALL, final - 3: MLP}
        for t in range(STEPS, STEPS + STAGES):
            for triple, first in firsts.items():
                k = t - first
                if k < STAGES:
                    run(k, triple, triple % 3, 2 if triple == final else 3, triple > final - 3)
                if triple == final and 7 <= k < STAGES - 1:
                    exchange(k - 7)

    return begin, tick, finish


def _mlp_step(i, b_ref, bt_ref, dy_ref, dyt_ref, wg_ref, wu_ref, wd_ref, h_ref, grad, db_s, dh_s, hid_s, dg_s, du_s):
    t = b_ref.shape[0]
    parts = [slice(r, r + D) for r in range(0, t, D)]

    @pl.when(i == 0)
    def _():
        db_s[...] = jnp.zeros_like(db_s)

    wg, wu, wd = wg_ref[0], wu_ref[0], wd_ref[0]
    for here in parts:
        gate, up = _dot(b_ref[here], wg), _dot(b_ref[here], wu)
        dh = _dot(dy_ref[here], wd, 1, 1).astype(BF16).astype(F32)
        sig = 0.5 * jnp.tanh(0.5 * gate) + 0.5
        act = gate * sig
        hid_s[here] = (act * up).astype(BF16)
        du_s[here] = (dh * act).astype(BF16)
        dg_s[here] = (dh * up * (sig + act * (1 - sig))).astype(BF16)
    for here in parts:
        db_s[here] += _dot(dg_s[here], wg, 1, 1) + _dot(du_s[here], wu, 1, 1)
    first, n = 3 * lax.div(i, 2), lax.rem(i, 2)
    grad[lax.rem(first, SLOTS), n] = _dot(bt_ref[...], dg_s[...]).astype(BF16)
    grad[lax.rem(first + 1, SLOTS), n] = _dot(bt_ref[...], du_s[...]).astype(BF16)
    grad[lax.rem(first + 2, SLOTS), n] = _dot(dyt_ref[...], hid_s[...]).astype(BF16)

    @pl.when(i == MLP - 1)
    def _():
        for here in parts:
            db = db_s[here].astype(BF16).astype(F32)
            wide = h_ref[here].astype(F32)
            scale = _norm_scale(wide)
            inner = jnp.mean(db * wide, -1, keepdims=True)
            dh_s[here] = (dy_ref[here].astype(F32) + (db * scale - wide * (scale * scale * scale * inner))).astype(BF16)


def _attend_step(g, sub, q_ref, k_ref, v_ref, ot_ref, lse_ref, wo_ref, at_ref, cos_ref, sin_ref, grad, dh_s, dot_s, delta_s, dq_s, dk_s, dv_s):
    t = q_ref.shape[0]
    heads = range(q_ref.shape[1] // HEAD)
    half = t // 2
    hidden = lax.broadcasted_iota(jnp.int32, (BQ, BQ), 0) > lax.broadcasted_iota(jnp.int32, (BQ, BQ), 1)
    first = lax.rem(CHUNKS - 2 * GROUPS + 2 * g, SLOTS)
    second = lax.rem(first + 1, SLOTS)

    def block(a, end, j):
        queries, keys = slice(a, end), slice(j, j + BQ)
        scores = [_dot(k_ref[keys, _col(i)], q_ref[queries, _col(i)], 1, 1) for i in heads]
        dps = [_dot(v_ref[keys, _col(i)], dot_s[_col(i), queries]) for i in heads]
        for i in heads:
            p = jnp.exp2(scores[i] * E2 - lse_ref[i : i + 1, queries])
            if a == j:
                cut = jnp.where(hidden, 0.0, p[:, :BQ])
                p = cut if end - a == BQ else jnp.concatenate([cut, p[:, BQ:]], axis=1)
            ds = (p * (dps[i] - delta_s[i : i + 1, queries])).astype(BF16)
            dv_s[keys, _col(i)] += _dot(p.astype(BF16), dot_s[_col(i), queries], 1, 1)
            dk_s[keys, _col(i)] += _dot(ds, q_ref[queries, _col(i)])
            dq_s[_col(i), queries] += _dot(k_ref[keys, _col(i)].T, ds)

    def turned_back(one):
        one = (one * SCALE).astype(BF16).astype(F32)
        return (one * cos_ref[...] - pltpu.roll(one, HEAD // 2, 1) * sin_ref[...]).astype(BF16)

    @pl.when(sub == 0)
    def _():
        dot_s[...] = _dot(wo_ref[0], dh_s[...], 1, 1).astype(BF16)
        grad[second, 1] = _dot(ot_ref[...], dh_s[...]).astype(BF16)
        for i in heads:
            delta_s[i : i + 1, :] = jnp.sum(dot_s[_col(i), :].astype(F32) * ot_ref[_col(i), :].astype(F32), axis=0, keepdims=True)
        for total in (dq_s, dk_s, dv_s):
            total[...] = jnp.zeros_like(total)
        for j in range(0, half, BQ):
            block(j, half, j)

    @pl.when(sub == 1)
    def _():
        for j in range(0, half, BQ):
            block(half, t, j)

    @pl.when(sub == 2)
    def _():
        for j in range(half, t, BQ):
            block(j, t, j)
        grad[second, 0] = _dot(at_ref[...], dv_s[...].astype(BF16)).astype(BF16)
        dk = jnp.concatenate([turned_back(dk_s[:, _col(i)]) for i in heads], axis=1)
        grad[first, 1] = _dot(at_ref[...], dk).astype(BF16)
        dq = jnp.concatenate([turned_back(dq_s[_col(i), :].T) for i in heads], axis=1)
        grad[first, 0] = _dot(at_ref[...], dq).astype(BF16)


def _backward_kernel(b_ref, bt_ref, dy_ref, dyt_ref, wg_ref, wu_ref, wd_ref, h_ref, q_ref, k_ref, v_ref, ot_ref, lse_ref, wo_ref, at_ref, cos_ref,
                     sin_ref, out_ref, sum_ref, dh_s, hid_s, dg_s, du_s, dot_s, delta_s, dq_s, dk_s, dv_s, grad, *rest):
    p = pl.program_id(0)
    begin, tick, finish = _reducer(grad, *rest, out_ref, sum_ref)
    pl.when(p == 0)(begin)
    tick(p)

    @pl.when(p < MLP)
    def _():
        _mlp_step(p, b_ref, bt_ref, dy_ref, dyt_ref, wg_ref, wu_ref, wd_ref, h_ref, grad, dk_s, dh_s, hid_s, dg_s, du_s)

    @pl.when(p >= MLP)
    def _():
        _attend_step(lax.div(p - MLP, SUBS), lax.rem(p - MLP, SUBS), q_ref, k_ref, v_ref, ot_ref, lse_ref, wo_ref, at_ref, cos_ref, sin_ref, grad, dh_s,
                     dot_s, delta_s, dq_s, dk_s, dv_s)

    pl.when(p == STEPS - 1)(finish)


def backward(b, bt, dy, dyt, wg, wu, wd, h, q, k, v, ot, lse, wo, at, cos, sin):
    t = b.shape[0]
    large = lambda p: jnp.minimum(p, MLP - 1)
    group = lambda p: lax.div(jnp.clip(p - MLP, 0, GROUPS * SUBS - 1), SUBS)
    cols = pl.BlockSpec((1, D, D), lambda p: (0, 0, large(p)))
    heads = pl.BlockSpec((t, D), lambda p: (0, group(p)))
    vm, sem = pltpu.VMEM, pltpu.SemaphoreType.DMA
    two = lambda *shape: vm((SLOTS, 2, 2) + shape, BF16)
    three = vm((SLOTS, 3, 2, PIECE, HEAD), BF16)
    return pl.pallas_call(
        _backward_kernel, grid=(STEPS,),
        in_specs=[_whole(t, D), _whole(D, t), _whole(t, D), _whole(D, t), cols, cols, pl.BlockSpec((1, D, D), lambda p: (0, large(p), 0)), _whole(t, D),
                  heads, heads, heads, pl.BlockSpec((D, t), lambda p: (group(p), 0)), pl.BlockSpec((None,) + lse.shape[1:], lambda p: (group(p), 0, 0)),
                  pl.BlockSpec((1, D, D), lambda p: (0, group(p), 0)), _whole(D, t), _whole(t, HEAD), _whole(t, HEAD)],
        out_specs=[pl.BlockSpec(memory_space=pl.ANY), pl.BlockSpec((PIECE, HEAD), lambda p: (0, 0))],
        out_shape=[jax.ShapeDtypeStruct((2 * CHUNKS, D, D), BF16), jax.ShapeDtypeStruct((PIECE, HEAD), F32)],
        scratch_shapes=[vm((t, D), BF16), vm((t, D), BF16), vm((t, D), BF16), vm((t, D), BF16), vm((D, t), BF16), vm((4, t), F32), vm((D, t), F32),
                        vm((t, D), F32), vm((t, D), F32), vm((SLOTS, 2, D, D), BF16), vm((SLOTS, 2, HALF, D), BF16), two(EIGHTH, D), two(EIGHTH, D),
                        two(QUARTER, D), two(QUARTER, D), vm((SLOTS, 2, QUARTER, D), F32), two(PIECE, HALF), two(PIECE, HALF), two(PIECE, D),
                        two(PIECE, D), vm((SLOTS, 2, PIECE, D), F32), three, three, vm((SLOTS, 2, PIECE, HEAD), BF16), vm((4, 4, PIECE, HEAD), F32),
                        vm((PIECE, HEAD), F32), sem((3,)), sem((STAGES - 1, 3)), sem((STAGES - 1, 3)), sem((2, 4, 3))],
        compiler_params=_params(collective_id=0, has_side_effects=True), cost_estimate=_cost(1.1e11, 1e8, 2e7),
    )(b, bt, dy, dyt, wg, wu, wd, h, q, k, v, ot, lse, wo, at, cos, sin)


AHEAD, BEHIND = 4, 4


def _adamw_kernel(count, sum_ref, g_ref, *refs):
    w, m, v, new_w, new_m, new_v = (refs[7 * i : 7 * i + 7] for i in range(6))
    g_s, w_s, m_s, v_s, out_w, out_m, out_v, isem, osem = refs[42:]
    factor = jnp.minimum(1.0, 0.5 * lax.rsqrt(jnp.sum(sum_ref[...], keepdims=True) / count + 1e-30))

    def part(ref, n, i):
        here = pl.ds(pl.multiple_of(i * D, D), D)
        return ref.at[0, here, :] if n in (3, 6) else ref.at[0, :, here]

    def fetch(n, i, slot):
        block = 6 * lax.div(i, 2) + lax.rem(i, 2) + 2 * (n - 4) if n > 3 else 3 * MLP + GROUPS * i + n
        return [pltpu.make_async_copy(src, dst.at[slot], isem.at[k, slot]) for k, (src, dst) in enumerate(
            ((g_ref.at[block], g_s), (part(w[n], n, i), w_s), (part(m[n], n, i), m_s), (part(v[n], n, i), v_s)))]

    def store(n, i, slot):
        return [pltpu.make_async_copy(src.at[slot], dst, osem.at[k, slot]) for k, (src, dst) in enumerate(
            ((out_w, part(new_w[n], n, i)), (out_m, part(new_m[n], n, i)), (out_v, part(new_v[n], n, i))))]

    def start(copies):
        for copy in copies:
            copy.start()

    def finish(copies):
        for copy in copies:
            copy.wait()

    def update(n, i, u):
        slot, out = lax.rem(u, AHEAD), lax.rem(u, BEHIND)
        finish(fetch(n, i, slot))
        pl.when(u >= BEHIND)(lambda: finish(store(n, i, out)))

        def some(r, _):
            here = pl.ds(pl.multiple_of(r * HEAD, HEAD), HEAD)
            gradient = (g_s[slot, :, here].T if n == 6 else g_s[slot, here, :]).astype(F32) * factor
            mean = 0.9 * m_s[slot, here, :] + 0.1 * gradient
            square = 0.95 * v_s[slot, here, :] + 0.05 * gradient * gradient
            weight = w_s[slot, here, :].astype(F32)
            step = mean * lax.rsqrt(square + 1e-8) + 0.1 * weight
            out_w[out, here, :] = (weight - 0.02 * step).astype(BF16)
            out_m[out, here, :] = mean
            out_v[out, here, :] = square

        lax.fori_loop(0, D // HEAD, some, None)
        start(store(n, i, out))

    for u in range(AHEAD):
        start(fetch(4 + u % 3, u // 3, u))

    def large(i, _):
        for k in range(3):
            u = 3 * i + k
            update(4 + k, i, u)
            n, later = (k + AHEAD) % 3, i + (k + AHEAD) // 3
            pl.when(later < MLP)(lambda: start(fetch(4 + n, later, lax.rem(u, AHEAD))))
            for e in range(n, AHEAD, 3):
                pl.when(later == MLP + e // 3)(lambda: start(fetch(e, 0, lax.rem(u, AHEAD))))

    def small(i, _):
        for n in range(4):
            u = 3 * MLP + 4 * i + n
            update(n, i, u)
            pl.when(i < GROUPS - 1)(lambda: start(fetch(n, i + 1, lax.rem(u, AHEAD))))

    lax.fori_loop(0, MLP, large, None)
    lax.fori_loop(0, GROUPS, small, None)
    for u in range(BEHIND):
        finish(store(0, 0, u))


def adamw(g, total, weights, m, v):
    shapes = [jax.ShapeDtypeStruct(w.shape, BF16) for w in weights] + [jax.ShapeDtypeStruct(w.shape, F32) for w in weights] * 2
    vm, sem = pltpu.VMEM, pltpu.SemaphoreType.DMA
    any_space = pl.BlockSpec(memory_space=pl.ANY)
    return pl.pallas_call(
        functools.partial(_adamw_kernel, float(sum(w.size for w in weights))),
        in_specs=[pl.BlockSpec(memory_space=vm)] + [any_space] * 22,
        out_specs=[any_space] * 21,
        out_shape=shapes,
        scratch_shapes=[vm((AHEAD, D, D), t) for t in (BF16, BF16, F32, F32)] + [vm((BEHIND, D, D), t) for t in (BF16, F32, F32)]
        + [sem((4, AHEAD)), sem((3, BEHIND))],
        compiler_params=pltpu.CompilerParams(vmem_limit_bytes=VMEM),
        cost_estimate=_cost(2.5e8, 3.7e8, 1.7e7),
    )(total, g, *weights, *m, *v)


def solution(mesh):
    def step(x, dy, *arrays):
        weights, m, v = (arrays[i : i + 7] for i in (0, 7, 14))
        wq, wk, wv, wo, w_gate, w_up, w_down = weights
        x, dy = x[0], dy[0]
        cos, sin = tables(x.shape[0])
        q, k, value, at, ot, lse, h, b, bt, dyt = front(x, dy, wq, wk, wv, wo, cos, sin)
        g, total = backward(b, bt, dy, dyt, w_gate, w_up, w_down, h, q, k, value, ot, lse, wo, at, cos, sin)
        return tuple(adamw(g, total, weights, m, v))

    states, all_of = P(("rep", "dp"), None, None), P(None, None, None)
    return jax.shard_map(
        step,
        mesh=mesh,
        in_specs=(states, states) + (all_of,) * 21,
        out_specs=(P("rep", None, None),) * 21,
        check_vma=False,
    )
```

```python
import functools

import jax
import jax.numpy as jnp
from jax import lax
from jax.experimental import pallas as pl
from jax.experimental.pallas import tpu as pltpu
from jax.sharding import PartitionSpec as P

F32, BF16 = jnp.float32, jnp.bfloat16
HIDDEN = -1e30
LOG2E = 1.4426950408889634
D, HALF, HEAD, QUARTER, EIGHTH, PIECE = 512, 256, 128, 64, 32, 16
THETA = 10000
VMEM = 63 * 2**20
ANY = "arbitrary"
MESH = pl.DeviceIdType.MESH
SCALE = HEAD**-0.5
E2 = SCALE * LOG2E


def _dot(a, b, ca=1, cb=0):
    return lax.dot_general(a, b, (((ca,), (cb,)), ((), ())), preferred_element_type=F32)


def _params(**more):
    return pltpu.CompilerParams(dimension_semantics=(ANY,), vmem_limit_bytes=VMEM, **more)


def _cost(flops, nbytes, exps=0):
    return pl.CostEstimate(flops=int(flops), bytes_accessed=int(nbytes), transcendentals=int(exps))


def _whole(*shape):
    return pl.BlockSpec(shape, lambda i: (0,) * len(shape), pipeline_mode=pl.Buffered(1))


def _col(i):
    return slice(i * HEAD, i * HEAD + HEAD)


def _norm_scale(wide):
    return lax.rsqrt(jnp.mean(wide * wide, -1, keepdims=True) + 1e-6)


def tables(tokens):
    half = HEAD // 2
    place = jnp.arange(HEAD)
    pace = THETA ** (-(place % half).astype(F32) / half)
    low = jnp.arange(EIGHTH, dtype=F32)[:, None] * pace
    high = (jnp.arange(tokens // EIGHTH, dtype=F32) * EIGHTH)[:, None] * pace
    sign = jnp.where(place < half, -1.0, 1.0)
    c, s, d, r = jnp.cos(high)[:, None], jnp.sin(high)[:, None], jnp.cos(low)[None], jnp.sin(low)[None]
    return (c * d - s * r).reshape(tokens, HEAD), ((s * d + c * r) * sign).reshape(tokens, HEAD)


BQ = HALF


def _front_kernel(x_ref, dy_ref, wq_ref, wk_ref, wv_ref, wo_ref, cos_ref, sin_ref, q_ref, k_ref, v_ref, at_ref, ot_ref, lse_ref, h_ref, b_ref, bt_ref,
                  dyt_ref, a_s, o_s, h_s, values_s):
    t = x_ref.shape[0]
    heads = range(D // HEAD)
    strips = [slice(r, r + BQ) for r in range(0, t, BQ)]

    @pl.when(pl.program_id(0) == 0)
    def _():
        for here in strips:
            wide = x_ref[here].astype(F32)
            a_s[here] = (wide * _norm_scale(wide)).astype(BF16)
        at_ref[...] = a_s[...].T
        dyt_ref[...] = dy_ref[...].T
        h_s[...] = jnp.zeros_like(h_s)
        for i in heads:
            values_s[i, HEAD:] = jnp.ones((PIECE, t), BF16)

    for here in strips:
        for w, out in ((wq_ref, q_ref), (wk_ref, k_ref)):
            whole = _dot(a_s[here], w[0]).astype(BF16).astype(F32)
            for i in heads:
                one = whole[:, _col(i)]
                out[here, _col(i)] = (one * cos_ref[here] + pltpu.roll(one, HEAD // 2, 1) * sin_ref[here]).astype(BF16)
        v_ref[here] = _dot(a_s[here], wv_ref[0]).astype(BF16)
    for i in heads:
        values_s[i, :HEAD] = v_ref[:, _col(i)].T

    hidden = lax.broadcasted_iota(jnp.int32, (BQ, BQ), 0) > lax.broadcasted_iota(jnp.int32, (BQ, BQ), 1)

    def scored(n):
        return [[_dot(k_ref[keys, _col(i)], q_ref[strips[n], _col(i)], 1, 1) for keys in strips[: n + 1]] for i in heads]

    ahead = scored(0)
    for n, here in enumerate(strips):
        scores, ahead = ahead, scored(n + 1) if n + 1 < len(strips) else None
        weights, tops = [], []
        for s in scores:
            s[n] = jnp.where(hidden, HIDDEN, s[n])
            top = functools.reduce(jnp.maximum, [one.max(axis=0, keepdims=True) for one in s]) * E2
            weights.append(jnp.concatenate([jnp.exp2(one * E2 - top).astype(BF16) for one in s], axis=0))
            tops.append(top)
        for i in heads:
            mix = _dot(values_s[i, :, : here.stop], weights[i])
            total = mix[HEAD : HEAD + 1]
            out = (mix[:HEAD] * (1 / total)).astype(BF16)
            ot_ref[_col(i), here] = out
            o_s[here, _col(i)] = out.T
            lse_ref[i : i + 1, here] = tops[i] + jnp.log2(total)
    for here in strips:
        h_s[here] += _dot(o_s[here], wo_ref[0])

    @pl.when(pl.program_id(0) == pl.num_programs(0) - 1)
    def _():
        for here in strips:
            h = (x_ref[here].astype(F32) + h_s[here].astype(BF16).astype(F32)).astype(BF16)
            h_ref[here] = h
            wide = h.astype(F32)
            b = (wide * _norm_scale(wide)).astype(BF16)
            b_ref[here] = b
            bt_ref[:, here] = b.T


def front(x, dy, wq, wk, wv, wo, cos, sin):
    t, width = x.shape[0], wq.shape[2]
    n = width // D
    cols = pl.BlockSpec((t, D), lambda i: (0, i))
    w = pl.BlockSpec((1, D, D), lambda i: (0, 0, i))
    last = lambda *shape: pl.BlockSpec(shape, lambda i: (0, 0))
    shape = jax.ShapeDtypeStruct
    vm = pltpu.VMEM
    return pl.pallas_call(
        _front_kernel, grid=(n,), in_specs=[_whole(t, D), _whole(t, D), w, w, w, pl.BlockSpec((1, D, D), lambda i: (0, i, 0)), _whole(t, HEAD), _whole(t, HEAD)],
        out_specs=[cols, cols, cols, last(D, t), pl.BlockSpec((D, t), lambda i: (i, 0)), pl.BlockSpec((None, D // HEAD, t), lambda i: (i, 0, 0)),
                   last(t, D), last(t, D), last(D, t), last(D, t)],
        out_shape=[shape((t, width), BF16)] * 3 + [shape((D, t), BF16), shape((width, t), BF16), shape((n, D // HEAD, t), F32), shape((t, D), BF16),
                                                   shape((t, D), BF16), shape((D, t), BF16), shape((D, t), BF16)],
        scratch_shapes=[vm((t, D), BF16), vm((t, D), BF16), vm((t, D), F32), vm((D // HEAD, HEAD + PIECE, t), BF16)],
        compiler_params=_params(), cost_estimate=_cost(1.8e10, 4e7, 1e7),
    )(x, dy, wq, wk, wv, wo, cos, sin)


STRIDE = (32, 8, 2)
MLP, GROUPS, SUBS = 16, 4, 3
STEPS = MLP + GROUPS * SUBS
CHUNKS = 32
STAGES = 13
SMALL = MLP + 2 * SUBS
NEXT = SMALL + SUBS + 1
SLOTS = 9


def _reducer(grad, rd, s1, r1, s2, r2, p1, s3, r3, s4, r4, p2, s5, r5, fin, ebuf, acc, dsem, ssem, rsem, esem, out_ref, sum_ref):
    me = lax.axis_index("dp")
    core = lax.rem(me, 2)
    pos = [lax.rem(lax.div(me, s), 4) for s in STRIDE]
    partner = me + 1 - 2 * core

    def at(q, o):
        return jnp.where(q < 4 - o, q + o, q + o - 4)

    def peer(d, o):
        return me + jnp.where(pos[d] < 4 - o, o * STRIDE[d], (o - 4) * STRIDE[d])

    def greet():
        barrier = pltpu.get_barrier_semaphore()
        for dev in [partner] + [peer(d, o) for d in range(3) for o in (1, 2, 3)]:
            pl.semaphore_signal(barrier, inc=1, device_id={"dp": dev}, device_id_type=MESH)
        acc[...] = jnp.zeros_like(acc)

    def begin():
        pl.semaphore_wait(pltpu.get_barrier_semaphore(), 10)

    rows = lambda start, n: pl.ds(pl.multiple_of(start, PIECE), n)
    lanes = lambda start, n: pl.ds(pl.multiple_of(start, HEAD), n)
    base = core * HALF

    def remote(src, dst, k, third, dev):
        return pltpu.make_async_remote_copy(src_ref=src, dst_ref=dst, send_sem=ssem.at[k, third], recv_sem=rsem.at[k, third],
                                            device_id={"dp": dev}, device_id_type=MESH)

    def wait(k, third, streams, late):
        same = (rd, r1, r2, r3, r4, r5, r5, r4, r3, r2, r1, rd)[k].at[pl.ds(3 * third, streams)]
        remote(same, same, k, third, partner).wait()
        if k == (11 if late else 6):
            same = (rd if late else fin).at[pl.ds(3 * third, streams)]
            pltpu.make_async_copy(same, same, dsem.at[third]).wait()

    def stream(j):
        d1, d2, d3 = j, (j + 1) % 3, (j + 2) % 3
        q1, q2, q3 = pos[d1], pos[d2], pos[d3]
        row1 = q1 * QUARTER
        row2 = row1 + q2 * PIECE

        def copies(k, c, third, late=False):
            s = 3 * third + j
            send = lambda src, dst, dev: remote(src, dst, k, third, dev)
            right1, left1, right2, left2 = peer(d1, 1), peer(d1, 3), peer(d2, 1), peer(d2, 3)

            def home(row, n, lane=pl.ds(0, D)):
                return rd.at[s, :, rows(row, n), lane] if late else out_ref.at[pl.ds(2 * c, 2), rows(base + row, n), lane]

            if k == 0:
                return [send(grad.at[s, :, rows(HALF - base, HALF), :], rd.at[s], partner)]
            if k in (1, 2, 3, 4):
                src, dst = ((s1, r1), (s2, r2), (s3, r3), (s4, r4))[k - 1]
                right, left = (right1, left1) if k < 3 else (right2, left2)
                return [send(src.at[s, 0], dst.at[s, 0], right), send(src.at[s, 1], dst.at[s, 1], left)]
            if k == 5:
                return [send(s5.at[s, o - 1], r5.at[s, o - 1], peer(d3, o)) for o in (1, 2, 3)]
            if k == 6:
                mine = home(row2, PIECE, lanes(q3 * HEAD, HEAD))
                own = [] if late else [pltpu.make_async_copy(fin.at[s], mine, dsem.at[third])]
                return own + [send(fin.at[s], mine, peer(d3, o)) for o in (1, 2, 3)]
            if k == 7:
                mine = home(row2, PIECE)
                return [send(mine, mine, right2), send(mine, mine, left2)]
            if k == 8:
                a = home(row1 + at(q2, 3) * PIECE, PIECE, pl.ds(0, HALF))
                z = home(row1 + at(q2, 1) * PIECE, PIECE, pl.ds(HALF, HALF))
                return [send(a, a, right2), send(z, z, left2)]
            if k == 9:
                mine = home(row1, QUARTER)
                return [send(mine, mine, right1), send(mine, mine, left1)]
            if k == 10:
                a = home(at(q1, 3) * QUARTER, EIGHTH)
                z = home(at(q1, 1) * QUARTER + EIGHTH, EIGHTH)
                return [send(a, a, right1), send(z, z, left1)]
            if k == 11:
                mine, goal = home(0, HALF), out_ref.at[pl.ds(2 * c, 2), rows(base, HALF), :]
                own = [pltpu.make_async_copy(mine, goal, dsem.at[third])] if late else []
                return own + [send(mine, goal, partner)]
            return []

        def work(k, s, late=False):
            def both(start, n):
                return grad[s, :, rows(base + start, n), :].astype(F32) + rd[s, :, rows(start, n), :].astype(F32)

            if k == 1:
                far = at(q1, 2) * QUARTER
                s1[s, 0] = both(far, EIGHTH).astype(BF16)
                s1[s, 1] = both(far + EIGHTH, EIGHTH).astype(BF16)
                p1[s] = both(q1 * QUARTER, QUARTER)
            if k == 2:
                a, z = at(q1, 1) * QUARTER, at(q1, 3) * QUARTER
                s2[s, 0, :, :EIGHTH] = (both(a, EIGHTH) + r1[s, 0].astype(F32)).astype(BF16)
                s2[s, 0, :, EIGHTH:] = both(a + EIGHTH, EIGHTH).astype(BF16)
                s2[s, 1, :, :EIGHTH] = both(z, EIGHTH).astype(BF16)
                s2[s, 1, :, EIGHTH:] = (both(z + EIGHTH, EIGHTH) + r1[s, 1].astype(F32)).astype(BF16)
            if k == 3:
                p1[s] += r2[s, 0].astype(F32) + r2[s, 1].astype(F32)
                far = p1[s, :, rows(at(q2, 2) * PIECE, PIECE), :].astype(BF16)
                s3[s, 0] = far[:, :, :HALF]
                s3[s, 1] = far[:, :, HALF:]
            if k == 4:
                a, z = p1[s, :, rows(at(q2, 1) * PIECE, PIECE), :], p1[s, :, rows(at(q2, 3) * PIECE, PIECE), :]
                s4[s, 0, :, :, :HALF] = (a[:, :, :HALF] + r3[s, 0].astype(F32)).astype(BF16)
                s4[s, 0, :, :, HALF:] = a[:, :, HALF:].astype(BF16)
                s4[s, 1, :, :, :HALF] = z[:, :, :HALF].astype(BF16)
                s4[s, 1, :, :, HALF:] = (z[:, :, HALF:] + r3[s, 1].astype(F32)).astype(BF16)
            if k == 5:
                p2[s] = p1[s, :, rows(q2 * PIECE, PIECE), :] + r4[s, 0].astype(F32) + r4[s, 1].astype(F32)
                for o in (1, 2, 3):
                    s5[s, o - 1] = p2[s, :, :, lanes(at(q3, o) * HEAD, HEAD)].astype(BF16)
            if k == 6:
                total = p2[s, :, :, lanes(q3 * HEAD, HEAD)]
                for o in (1, 2, 3):
                    total += r5[s, o - 1].astype(F32)
                total = total.astype(BF16)
                fin[s] = total
                if late:
                    rd[s, :, rows(row2, PIECE), lanes(q3 * HEAD, HEAD)] = total
                square = total.astype(F32) * total.astype(F32)
                acc[...] += square[0] + square[1]

        return copies, work

    streams = [stream(j) for j in range(3)]

    def run(k, triple, third, number=3, late=False):
        if k > 0:
            wait(k - 1, third, number, late)
        for j in range(number):
            streams[j][1](k, 3 * third + j, late)
        for j in range(number):
            for copy in streams[j][0](k, 3 * triple + j, third, late):
                copy.start()

    def stage(t, k):
        u = t - k
        now = (u >= 2) & (u <= MLP)
        if k + SMALL < STEPS:
            now = now | (u == SMALL)
        if k + NEXT < STEPS:
            now = now | (u == NEXT)

        @pl.when(now)
        def _():
            triple = jnp.where(u <= MLP, lax.div(u, 2) - 1, MLP // 2 + jnp.where(u > SMALL, 1, 0))
            run(k, triple, lax.rem(triple, 3))

    def hops(k):
        if k == 3:
            return [(0, core, partner)]
        return [(o - 1, pos[k], peer(k, o)) for o in (1, 2, 3)]

    def moves(k):
        return [pltpu.make_async_remote_copy(src_ref=ebuf.at[k, place], dst_ref=ebuf.at[k, place], send_sem=esem.at[0, k, n],
                                             recv_sem=esem.at[1, k, n], device_id={"dp": dev}, device_id_type=MESH)
                for n, place, dev in hops(k)]

    def exchange(k):
        if k > 0:
            for copy in moves(k - 1):
                copy.wait()
            total = ebuf[k - 1, 0] + ebuf[k - 1, 1]
            if k < 4:
                total = total + ebuf[k - 1, 2] + ebuf[k - 1, 3]
        else:
            total = acc[...]
        if k == 4:
            sum_ref[...] = total
        else:
            ebuf[k, hops(k)[0][1]] = total
            for copy in moves(k):
                copy.start()

    def tick(t):
        for odd in (0, 1):

            @pl.when(lax.rem(t, 2) == odd)
            def _():
                for k in range(STAGES - 2 + (1 - odd), -1, -2):
                    stage(t, k)

    def finish():
        final = MLP // 2 + 2
        firsts = {final: STEPS, final - 1: NEXT, final - 2: SMALL, final - 3: MLP}
        for t in range(STEPS, STEPS + STAGES):
            for triple, first in firsts.items():
                k = t - first
                if k < STAGES:
                    run(k, triple, triple % 3, 2 if triple == final else 3, triple > final - 3)
                if triple == final and 7 <= k < STAGES - 1:
                    exchange(k - 7)

    return greet, begin, tick, finish


def _mlp_step(i, b_ref, bt_ref, dy_ref, dyt_ref, wg_ref, wu_ref, wd_ref, h_ref, grad, db_s, dh_s, hid_s, dg_s, du_s):
    t = b_ref.shape[0]
    parts = [slice(r, r + D) for r in range(0, t, D)]

    @pl.when(i == 0)
    def _():
        db_s[...] = jnp.zeros_like(db_s)

    wg, wu, wd = wg_ref[0], wu_ref[0], wd_ref[0]
    for here in parts:
        gate, up = _dot(b_ref[here], wg), _dot(b_ref[here], wu)
        dh = _dot(dy_ref[here], wd, 1, 1).astype(BF16).astype(F32)
        sig = 0.5 * jnp.tanh(0.5 * gate) + 0.5
        act = gate * sig
        hid_s[here] = (act * up).astype(BF16)
        du_s[here] = (dh * act).astype(BF16)
        dg_s[here] = (dh * up * (sig + act * (1 - sig))).astype(BF16)
    for here in parts:
        db_s[here] += _dot(jnp.concatenate([dg_s[here], du_s[here]], 1), jnp.concatenate([wg, wu], 1), 1, 1)
    first, n = 3 * lax.div(i, 2), lax.rem(i, 2)
    grad[lax.rem(first, SLOTS), n] = _dot(bt_ref[...], dg_s[...]).astype(BF16)
    grad[lax.rem(first + 1, SLOTS), n] = _dot(bt_ref[...], du_s[...]).astype(BF16)
    grad[lax.rem(first + 2, SLOTS), n] = _dot(dyt_ref[...], hid_s[...]).astype(BF16)

    @pl.when(i == MLP - 1)
    def _():
        for here in parts:
            db = db_s[here].astype(BF16).astype(F32)
            wide = h_ref[here].astype(F32)
            scale = _norm_scale(wide)
            inner = jnp.mean(db * wide, -1, keepdims=True)
            dh_s[here] = (dy_ref[here].astype(F32) + (db * scale - wide * (scale * scale * scale * inner))).astype(BF16)


def _attend_step(g, sub, q_ref, k_ref, v_ref, ot_ref, lse_ref, wo_ref, at_ref, cos_ref, sin_ref, grad, dh_s, dot_s, delta_s, dq_s, dk_s, dv_s):
    t = q_ref.shape[0]
    heads = range(q_ref.shape[1] // HEAD)
    half = t // 2
    hidden = lax.broadcasted_iota(jnp.int32, (BQ, BQ), 0) > lax.broadcasted_iota(jnp.int32, (BQ, BQ), 1)
    first = lax.rem(CHUNKS - 2 * GROUPS + 2 * g, SLOTS)
    second = lax.rem(first + 1, SLOTS)

    def block(a, end, j):
        queries, keys = slice(a, end), slice(j, j + BQ)
        scores = [_dot(k_ref[keys, _col(i)], q_ref[queries, _col(i)], 1, 1) for i in heads]
        dps = [_dot(v_ref[keys, _col(i)], dot_s[_col(i), queries]) for i in heads]
        for i in heads:
            p = jnp.exp2(scores[i] * E2 - lse_ref[i : i + 1, queries])
            if a == j:
                cut = jnp.where(hidden, 0.0, p[:, :BQ])
                p = cut if end - a == BQ else jnp.concatenate([cut, p[:, BQ:]], axis=1)
            ds = (p * (dps[i] - delta_s[i : i + 1, queries])).astype(BF16)
            dv_s[keys, _col(i)] += _dot(p.astype(BF16), dot_s[_col(i), queries], 1, 1)
            dk_s[keys, _col(i)] += _dot(ds, q_ref[queries, _col(i)])
            dq_s[_col(i), queries] += _dot(k_ref[keys, _col(i)].T, ds)

    def turned_back(one):
        one = (one * SCALE).astype(BF16).astype(F32)
        return (one * cos_ref[...] - pltpu.roll(one, HEAD // 2, 1) * sin_ref[...]).astype(BF16)

    @pl.when(sub == 0)
    def _():
        dot_s[...] = _dot(wo_ref[0], dh_s[...], 1, 1).astype(BF16)
        grad[second, 1] = _dot(ot_ref[...], dh_s[...]).astype(BF16)
        for i in heads:
            delta_s[i : i + 1, :] = jnp.sum(dot_s[_col(i), :].astype(F32) * ot_ref[_col(i), :].astype(F32), axis=0, keepdims=True)
        for total in (dq_s, dk_s, dv_s):
            total[...] = jnp.zeros_like(total)
        for j in range(0, half, BQ):
            block(j, half, j)

    @pl.when(sub == 1)
    def _():
        for j in range(0, half, BQ):
            block(half, t, j)

    @pl.when(sub == 2)
    def _():
        for j in range(half, t, BQ):
            block(j, t, j)
        grad[second, 0] = _dot(at_ref[...], dv_s[...].astype(BF16)).astype(BF16)
        dk = jnp.concatenate([turned_back(dk_s[:, _col(i)]) for i in heads], axis=1)
        grad[first, 1] = _dot(at_ref[...], dk).astype(BF16)
        dq = jnp.concatenate([turned_back(dq_s[_col(i), :].T) for i in heads], axis=1)
        grad[first, 0] = _dot(at_ref[...], dq).astype(BF16)


def _backward_kernel(b_ref, bt_ref, dy_ref, dyt_ref, wg_ref, wu_ref, wd_ref, h_ref, q_ref, k_ref, v_ref, ot_ref, lse_ref, wo_ref, at_ref, cos_ref,
                     sin_ref, out_ref, sum_ref, dh_s, hid_s, dg_s, du_s, dot_s, delta_s, dq_s, dk_s, dv_s, grad, *rest):
    p = pl.program_id(0)
    greet, begin, tick, finish = _reducer(grad, *rest, out_ref, sum_ref)
    pl.when(p == 0)(greet)
    pl.when(p == 1)(begin)
    tick(p)

    @pl.when(p < MLP)
    def _():
        _mlp_step(p, b_ref, bt_ref, dy_ref, dyt_ref, wg_ref, wu_ref, wd_ref, h_ref, grad, dk_s, dh_s, hid_s, dg_s, du_s)

    @pl.when(p >= MLP)
    def _():
        _attend_step(lax.div(p - MLP, SUBS), lax.rem(p - MLP, SUBS), q_ref, k_ref, v_ref, ot_ref, lse_ref, wo_ref, at_ref, cos_ref, sin_ref, grad, dh_s,
                     dot_s, delta_s, dq_s, dk_s, dv_s)

    pl.when(p == STEPS - 1)(finish)


def backward(b, bt, dy, dyt, wg, wu, wd, h, q, k, v, ot, lse, wo, at, cos, sin):
    t = b.shape[0]
    large = lambda p: jnp.minimum(p, MLP - 1)
    group = lambda p: lax.div(jnp.clip(p - MLP, 0, GROUPS * SUBS - 1), SUBS)
    cols = pl.BlockSpec((1, D, D), lambda p: (0, 0, large(p)))
    heads = pl.BlockSpec((t, D), lambda p: (0, group(p)))
    vm, sem = pltpu.VMEM, pltpu.SemaphoreType.DMA
    two = lambda *shape: vm((SLOTS, 2, 2) + shape, BF16)
    three = vm((SLOTS, 3, 2, PIECE, HEAD), BF16)
    return pl.pallas_call(
        _backward_kernel, grid=(STEPS,),
        in_specs=[_whole(t, D), _whole(D, t), _whole(t, D), _whole(D, t), cols, cols, pl.BlockSpec((1, D, D), lambda p: (0, large(p), 0)), _whole(t, D),
                  heads, heads, heads, pl.BlockSpec((D, t), lambda p: (group(p), 0)), pl.BlockSpec((None,) + lse.shape[1:], lambda p: (group(p), 0, 0)),
                  pl.BlockSpec((1, D, D), lambda p: (0, group(p), 0)), _whole(D, t), _whole(t, HEAD), _whole(t, HEAD)],
        out_specs=[pl.BlockSpec(memory_space=pl.ANY), pl.BlockSpec((PIECE, HEAD), lambda p: (0, 0))],
        out_shape=[jax.ShapeDtypeStruct((2 * CHUNKS, D, D), BF16), jax.ShapeDtypeStruct((PIECE, HEAD), F32)],
        scratch_shapes=[vm((t, D), BF16), vm((t, D), BF16), vm((t, D), BF16), vm((t, D), BF16), vm((D, t), BF16), vm((4, t), F32), vm((D, t), F32),
                        vm((t, D), F32), vm((t, D), F32), vm((SLOTS, 2, D, D), BF16), vm((SLOTS, 2, HALF, D), BF16), two(EIGHTH, D), two(EIGHTH, D),
                        two(QUARTER, D), two(QUARTER, D), vm((SLOTS, 2, QUARTER, D), F32), two(PIECE, HALF), two(PIECE, HALF), two(PIECE, D),
                        two(PIECE, D), vm((SLOTS, 2, PIECE, D), F32), three, three, vm((SLOTS, 2, PIECE, HEAD), BF16), vm((4, 4, PIECE, HEAD), F32),
                        vm((PIECE, HEAD), F32), sem((3,)), sem((STAGES - 1, 3)), sem((STAGES - 1, 3)), sem((2, 4, 3))],
        compiler_params=_params(collective_id=0, has_side_effects=True), cost_estimate=_cost(1.1e11, 1e8, 2e7),
    )(b, bt, dy, dyt, wg, wu, wd, h, q, k, v, ot, lse, wo, at, cos, sin)


AHEAD, BEHIND = 4, 4


def _adamw_kernel(count, sum_ref, g_ref, *refs):
    w, m, v, new_w, new_m, new_v = (refs[7 * i : 7 * i + 7] for i in range(6))
    g_s, w_s, m_s, v_s, out_w, out_m, out_v, isem, osem = refs[42:]
    factor = jnp.minimum(1.0, 0.5 * lax.rsqrt(jnp.sum(sum_ref[...], keepdims=True) / count + 1e-30))

    def part(ref, n, i):
        here = pl.ds(pl.multiple_of(i * D, D), D)
        return ref.at[0, here, :] if n in (3, 6) else ref.at[0, :, here]

    def fetch(n, i, slot):
        block = 6 * lax.div(i, 2) + lax.rem(i, 2) + 2 * (n - 4) if n > 3 else 3 * MLP + GROUPS * i + n
        return [pltpu.make_async_copy(src, dst.at[slot], isem.at[k, slot]) for k, (src, dst) in enumerate(
            ((g_ref.at[block], g_s), (part(w[n], n, i), w_s), (part(m[n], n, i), m_s), (part(v[n], n, i), v_s)))]

    def store(n, i, slot):
        return [pltpu.make_async_copy(src.at[slot], dst, osem.at[k, slot]) for k, (src, dst) in enumerate(
            ((out_w, part(new_w[n], n, i)), (out_m, part(new_m[n], n, i)), (out_v, part(new_v[n], n, i))))]

    def start(copies):
        for copy in copies:
            copy.start()

    def finish(copies):
        for copy in copies:
            copy.wait()

    def update(n, i, u):
        slot, out = lax.rem(u, AHEAD), lax.rem(u, BEHIND)
        finish(fetch(n, i, slot))
        pl.when(u >= BEHIND)(lambda: finish(store(n, i, out)))

        def some(r, _):
            here = pl.ds(pl.multiple_of(r * HEAD, HEAD), HEAD)
            gradient = (g_s[slot, :, here].T if n == 6 else g_s[slot, here, :]).astype(F32) * factor
            mean = 0.9 * m_s[slot, here, :] + 0.1 * gradient
            square = 0.95 * v_s[slot, here, :] + 0.05 * gradient * gradient
            weight = w_s[slot, here, :].astype(F32)
            step = mean * lax.rsqrt(square + 1e-8) + 0.1 * weight
            out_w[out, here, :] = (weight - 0.02 * step).astype(BF16)
            out_m[out, here, :] = mean
            out_v[out, here, :] = square

        lax.fori_loop(0, D // HEAD, some, None)
        start(store(n, i, out))

    for u in range(AHEAD):
        start(fetch(4 + u % 3, u // 3, u))

    def large(i, _):
        for k in range(3):
            u = 3 * i + k
            update(4 + k, i, u)
            n, later = (k + AHEAD) % 3, i + (k + AHEAD) // 3
            pl.when(later < MLP)(lambda: start(fetch(4 + n, later, lax.rem(u, AHEAD))))
            for e in range(n, AHEAD, 3):
                pl.when(later == MLP + e // 3)(lambda: start(fetch(e, 0, lax.rem(u, AHEAD))))

    def small(i, _):
        for n in range(4):
            u = 3 * MLP + 4 * i + n
            update(n, i, u)
            pl.when(i < GROUPS - 1)(lambda: start(fetch(n, i + 1, lax.rem(u, AHEAD))))

    lax.fori_loop(0, MLP, large, None)
    lax.fori_loop(0, GROUPS, small, None)
    for u in range(BEHIND):
        finish(store(0, 0, u))


def adamw(g, total, weights, m, v):
    shapes = [jax.ShapeDtypeStruct(w.shape, BF16) for w in weights] + [jax.ShapeDtypeStruct(w.shape, F32) for w in weights] * 2
    vm, sem = pltpu.VMEM, pltpu.SemaphoreType.DMA
    any_space = pl.BlockSpec(memory_space=pl.ANY)
    return pl.pallas_call(
        functools.partial(_adamw_kernel, float(sum(w.size for w in weights))),
        in_specs=[pl.BlockSpec(memory_space=vm)] + [any_space] * 22,
        out_specs=[any_space] * 21,
        out_shape=shapes,
        scratch_shapes=[vm((AHEAD, D, D), t) for t in (BF16, BF16, F32, F32)] + [vm((BEHIND, D, D), t) for t in (BF16, F32, F32)]
        + [sem((4, AHEAD)), sem((3, BEHIND))],
        compiler_params=pltpu.CompilerParams(vmem_limit_bytes=VMEM),
        cost_estimate=_cost(2.5e8, 3.7e8, 1.7e7),
    )(total, g, *weights, *m, *v)


def solution(mesh):
    def step(x, dy, *arrays):
        weights, m, v = (arrays[i : i + 7] for i in (0, 7, 14))
        wq, wk, wv, wo, w_gate, w_up, w_down = weights
        x, dy = x[0], dy[0]
        cos, sin = tables(x.shape[0])
        q, k, value, at, ot, lse, h, b, bt, dyt = front(x, dy, wq, wk, wv, wo, cos, sin)
        g, total = backward(b, bt, dy, dyt, w_gate, w_up, w_down, h, q, k, value, ot, lse, wo, at, cos, sin)
        return tuple(adamw(g, total, weights, m, v))

    states, all_of = P(("rep", "dp"), None, None), P(None, None, None)
    return jax.shard_map(
        step,
        mesh=mesh,
        in_specs=(states, states) + (all_of,) * 21,
        out_specs=(P("rep", None, None),) * 21,
        check_vma=False,
    )
```
